32 devices in a mesh: expert: 16 (over z, y, x), tensor: 2 (over core).
Axes of the slice: x: 2, y: 2, z: 4, core: 2. Of those that a mesh axis runs over, the one named last changes fastest.
Arguments:
- tokens: bfloat16 [8192, 2048], P('expert'), may hold values from -6 to 6
- attn_gain: bfloat16 [2048], P('expert'), may hold values from 0.099609375 to 1.8984375
- moe_gain: bfloat16 [2048], P('expert'), may hold values from 0.099609375 to 1.8984375
- query_gain: bfloat16 [128], P('expert'), may hold values from 0.5 to 4.5
- key_gain: bfloat16 [128], P('expert'), may hold values from 0.5 to 4.5
- query_weight: bfloat16 [2048, 4096], P('expert', 'tensor'), may hold values from -0.088388348 to 0.088388348
- key_weight: bfloat16 [2048, 512], P('expert', 'tensor'), may hold values from -0.088388348 to 0.088388348
- value_matrix: bfloat16 [2048, 512], P('expert', 'tensor'), may hold values from -0.125 to 0.125
- output_weight: bfloat16 [2048, 4096], P('expert', 'tensor'), may hold values from -0.375 to 0.375
- gate_proj: bfloat16 [32, 2048, 768], P('expert', None, 'tensor'), may hold values from -0.125 to 0.125
- up_proj: bfloat16 [32, 2048, 768], P('expert', None, 'tensor'), may hold values from -0.125 to 0.125
- down_proj: bfloat16 [32, 768, 2048], P('expert', 'tensor'), may hold values from -0.875 to 0.875
- gate_weights: float32 [8192, 8], P('expert'), may hold values from 0.05 to 0.25
- routes: int32 [8192, 8], P('expert'), may hold values from 0 to 31, all different within a row; in each aligned block of 512 rows (0 to 511, 512 to 1023, ...) at most 160 rows name the same one
- doc_start: int32 [8192], P('expert'), may hold values from 0 to 1, as said below
- cotangent: bfloat16 [8192, 2048], P('expert'), may hold values from -6 to 6
Outputs:
- block_out: bfloat16 [8192, 2048], P('expert')
- grad_tokens: float32 [8192, 2048], P('expert')
- grad_query: float32 [2048, 4096], P('expert', 'tensor')
- grad_key: float32 [2048, 512], P('expert', 'tensor')
- grad_value: float32 [2048, 512], P('expert', 'tensor')
- grad_output: float32 [2048, 4096], P('expert', 'tensor')
- grad_attn_gain: float32 [2048], P('expert')
- grad_moe_gain: float32 [2048], P('expert')
- grad_query_gain: float32 [128], P('expert')
- grad_key_gain: float32 [128], P('expert')
- grad_gate_proj: float32 [32, 2048, 768], P('expert', None, 'tensor')
- grad_up_proj: float32 [32, 2048, 768], P('expert', None, 'tensor')
- grad_down_proj: float32 [32, 768, 2048], P('expert', 'tensor')
- grad_gates: float32 [8192, 8], P('expert')
The draws below stay inside these ranges and needn't reach their ends.
Inputs may be any that keep to these rules, and one draw needn't show every extreme that they name: `routes`: in each device's 512 rows no expert is named by more than 160 rows, a bound that some block reaches. `doc_start`: each block of 512 rows begins with 1, so documents never cross blocks; some block holds a single document of 512 rows.
All inputs are finite; a program needn't handle non-finite values.
Results may differ from the reference program's by a relative error of at most 0.015.
The reference program's roundings to bfloat16 on the way count: a program that leaves them out, or rounds other values in their place, can miss the bound.
Values may be sent and summed in bfloat16 or wider, within the bound.
A program may use at most 384 MiB of HBM per device.

```python
import math
import jax
import jax.numpy as jnp
import numpy as np
from jax import lax

MODEL_WIDTH = 2048
QUERY_HEADS = 32
KEY_VALUE_HEADS = 4
HEAD_SIZE = 128
FFE = 768
TOPK = 8
TOKENS_PER_SHARD = 512
EXPERTS = 32
MOST = 160
TOKEN_COUNT = 8192
N_TENSOR = 2


def query_unrotated(key):
    shape = (MODEL_WIDTH, QUERY_HEADS * HEAD_SIZE)
    value_heads_out = jnp.clip(jax.random.normal(jax.random.fold_in(key, 11), shape, jnp.float32), -4.0, 4.0)
    return value_heads_out * (1.0 / math.sqrt(MODEL_WIDTH))


def draw_query_weight(key, part):
    return query_unrotated(key).astype(jnp.bfloat16)


def draw_key_weight(key, part):
    value_heads_out = jnp.clip(jax.random.normal(jax.random.fold_in(key, 12), (MODEL_WIDTH, KEY_VALUE_HEADS * HEAD_SIZE), jnp.float32), -4.0, 4.0)
    return (value_heads_out * (1.0 / math.sqrt(MODEL_WIDTH))).astype(jnp.bfloat16)


def draw_query_gain(key, part):
    return jax.random.uniform(jax.random.fold_in(key, 21), (HEAD_SIZE,), jnp.float32, 0.6, 1.4).astype(jnp.bfloat16)


def draw_key_gain(key, part):
    return jax.random.uniform(jax.random.fold_in(key, 22), (HEAD_SIZE,), jnp.float32, 0.6, 1.4).astype(jnp.bfloat16)


def draw_doc_start(key, part):
    block_list = TOKEN_COUNT // TOKENS_PER_SHARD
    rate_key = jax.random.fold_in(key, 31)
    flag_key = jax.random.fold_in(key, 32)
    single_key = jax.random.fold_in(key, 33)
    inverse_rate = jax.random.randint(rate_key, (block_list, 1), 8, 257)
    draws_int = jax.random.randint(flag_key, (block_list, TOKENS_PER_SHARD), 0, 1048576)
    flags = draws_int % inverse_rate == 0
    single = jax.random.randint(single_key, (), 0, block_list)
    row_index = jnp.arange(block_list, dtype=jnp.int32)[:, None]
    col_index = jnp.arange(TOKENS_PER_SHARD, dtype=jnp.int32)[None, :]
    flags = jnp.where(row_index == single, False, flags)
    flags = jnp.where(col_index == 0, True, flags)
    return flags.astype(jnp.int32).reshape(TOKEN_COUNT)


def spiked(values, own_key, source, target, parts, factor):
    owner, partner = [(jnp.arange(values.shape[position]) // (values.shape[position] // parts)).reshape([-1 if axis == position else 1 for axis in range(values.ndim)]) for position in (source, target)]
    chosen = jax.random.permutation(own_key, parts)[partner]
    strong = (owner == chosen) | (owner == (partner + parts // 2) % parts)
    return jnp.where(strong, factor * values, values)


def shard_levels(key, extent, shards, least, top_value):
    def one(axis_at, blocks):
        heights = jax.random.uniform(jax.random.fold_in(jax.random.fold_in(key, 6), axis_at), (blocks,), jnp.float32, least / len(shards), top_value / len(shards))
        return jnp.repeat(jnp.exp(heights), extent[axis_at] // blocks).reshape((-1,) + (1,) * (len(extent) - axis_at - 1))

    loudness = one(*shards[0])
    for cut in shards[1:]:
        loudness = loudness * one(*cut)
    return loudness


def shared_out(rng, own, number, rows, number_of, top, reach, lean):
    ranking = jax.random.permutation(rng, number_of)
    crowded, ordinary = shares(number_of, rows * top, reach, lean, True), shares(number_of, rows * top, reach, lean, False)
    places = jnp.arange(number_of)

    def named(tallies, turn):
        used = int((tallies > 0).sum())
        fixed = max(1, used // 4)
        shifted = fixed + (places - fixed + turn * (used - fixed)) % max(1, number_of - fixed)
        return jnp.zeros((number_of,), jnp.int32).at[ranking[jnp.where(places < fixed, places, shifted)]].set(jnp.asarray(tallies, jnp.int32))

    tallies = jnp.where(number % 4 == 0, named(crowded, number // 4), named(ordinary, number - number // 4 - 1))
    mixed = jax.random.permutation(jax.random.fold_in(own, 3), number_of)
    source_of, taker = mixed[0:number_of // 2 * 2:2], mixed[1:number_of // 2 * 2:2]
    room = jnp.minimum(tallies[source_of] - 1, reach - tallies[taker]) // 2
    room = jnp.where((source_of == ranking[0]) | (taker == ranking[0]) | (tallies[taker] == 0), 0, jnp.maximum(room, 0))
    shifted = jax.random.randint(jax.random.fold_in(own, 4), (number_of // 2,), 0, 1 << 20) % (room + 1)
    tallies = tallies.at[source_of].add(-shifted).at[taker].add(shifted)
    labels = jnp.searchsorted(jnp.cumsum(tallies), jnp.arange(rows * top), side="right").astype(jnp.int32)
    table = labels.reshape(top, rows).T
    table = table[jax.random.permutation(jax.random.fold_in(own, 1), rows)]
    turn = jax.random.randint(jax.random.fold_in(own, 2), (rows, 1), 0, top)
    return jnp.take_along_axis(table, (jnp.arange(top)[None, :] + turn) % top, axis=1)


def shares(amount, total, reach, skew, full):
    loads = [(1 << 20) // math.isqrt(standing ** skew) + 1 for standing in range(1, amount + 1)]
    largest = reach if full else min(reach, max(-(-total // amount), total * loads[0] // sum(loads)))
    least = 1 if total - largest >= amount - 1 else 0
    holding, rest = [largest] + [least] * (amount - 1), total - largest - least * (amount - 1)
    while rest > 0:
        free = [i for i in range(1, amount) if holding[i] < largest] or [i for i in range(1, amount) if holding[i] < reach]
        pool, remaining = sum([loads[i] for i in free]), rest
        for i in free:
            extra = min(reach - holding[i], max(1, remaining * loads[i] // pool), rest)
            holding[i] = holding[i] + extra
            rest = rest - extra
    return np.array(holding)


def bell_draw(own_key, shape, deviation, reach, pieces=(), kind=jnp.bfloat16):
    entries = deviation * jax.random.normal(own_key, shape, jnp.float32)
    if pieces:
        entries = entries * shard_levels(own_key, shape, pieces, -0.22, 0.18)
    return jnp.clip(entries, -reach, reach).astype(kind)


def noise_with(key, dims, deviation, reach, pieces, heavy, kind=jnp.bfloat16):
    values = deviation * jax.random.normal(key, dims, jnp.float32)
    if pieces:
        values = values * shard_levels(key, dims, pieces, -0.22, 0.18)
    return jnp.clip(spiked(values, jax.random.fold_in(key, 3), *heavy), -reach, reach).astype(kind)


def setup_inputs(seed: int = 0) -> dict:
    seeds = jax.random.split(jax.random.key(seed), 17)
    tokens = bell_draw(seeds[0], (TOKEN_COUNT, MODEL_WIDTH), 1.0, 6.0, ((0, 16),))
    attn_gain = jnp.clip(1.0 + 0.18 * jax.random.normal(seeds[1], (MODEL_WIDTH,), jnp.float32), 0.099609375, 1.8984375).astype(jnp.bfloat16)
    moe_gain = jnp.clip(1.0 + 0.18 * jax.random.normal(seeds[2], (MODEL_WIDTH,), jnp.float32), 0.099609375, 1.8984375).astype(jnp.bfloat16)
    query_gain = draw_query_gain(jax.random.fold_in(seeds[16], 71), 0)
    key_gain = draw_key_gain(jax.random.fold_in(seeds[16], 71), 0)
    query_weight = draw_query_weight(jax.random.fold_in(seeds[16], 71), 0)
    key_weight = draw_key_weight(jax.random.fold_in(seeds[16], 71), 0)
    value_matrix = bell_draw(seeds[7], (MODEL_WIDTH, KEY_VALUE_HEADS * HEAD_SIZE), MODEL_WIDTH ** -0.5, 0.125, ((0, 16), (1, 2)))
    output_weight = bell_draw(seeds[8], (MODEL_WIDTH, QUERY_HEADS * HEAD_SIZE), (QUERY_HEADS * HEAD_SIZE // 16) ** -0.5, 0.375, ((0, 16), (1, 2)))
    gate_proj = bell_draw(seeds[9], (EXPERTS, MODEL_WIDTH, FFE), MODEL_WIDTH ** -0.5, 0.125, ((0, 16), (2, 2)))
    up_proj = bell_draw(seeds[10], (EXPERTS, MODEL_WIDTH, FFE), MODEL_WIDTH ** -0.5, 0.125, ((0, 16), (2, 2)))
    down_proj = bell_draw(seeds[11], (EXPERTS, FFE, MODEL_WIDTH), (FFE // 16) ** -0.5, 0.875, ((0, 16), (1, 2)))
    gate_weights = jnp.clip(0.05 + 0.2 * jax.random.uniform(seeds[12], (TOKEN_COUNT, TOPK), jnp.float32) ** shard_levels(seeds[12], (TOKEN_COUNT, TOPK), ((0, 16),), -0.2, 0.2), 0.05, 0.25)
    routes_keys = jax.random.split(jax.random.fold_in(seeds[13], 1), TOKEN_COUNT // TOKENS_PER_SHARD)
    routes_turns = jax.random.permutation(jax.random.fold_in(seeds[13], 3), TOKEN_COUNT // TOKENS_PER_SHARD)
    routes = jax.vmap(lambda own, number: shared_out(jax.random.fold_in(seeds[13], 2), own, number, TOKENS_PER_SHARD, EXPERTS, TOPK, MOST, 2))(routes_keys, routes_turns).reshape((TOKEN_COUNT, TOPK))
    doc_start = draw_doc_start(jax.random.fold_in(seeds[16], 71), 0)
    cotangent = noise_with(seeds[15], (TOKEN_COUNT, MODEL_WIDTH), 1.0, 6.0, ((0, 16),), (0, 1, 16, 2.0))
    return {"tokens": tokens, "attn_gain": attn_gain, "moe_gain": moe_gain, "query_gain": query_gain, "key_gain": key_gain, "query_weight": query_weight, "key_weight": key_weight, "value_matrix": value_matrix, "output_weight": output_weight, "gate_proj": gate_proj, "up_proj": up_proj, "down_proj": down_proj, "gate_weights": gate_weights, "routes": routes, "doc_start": doc_start, "cotangent": cotangent}


EPS = 1e-06
NEG = -1e+30
THETA = 1000000.0

@jax.custom_vjp
def reduced_precision(v):
    return lax.optimization_barrier(v.astype(jnp.bfloat16)).astype(jnp.float32)

@jax.custom_vjp
def reduced_backward(v):
    return v

def low_keep(v):
    return (reduced_precision(v), None)

def low_pass(kept, grad):
    return (grad,)

def back_keep(v):
    return (v, None)

def back_low(kept, grad):
    return (reduced_precision(grad),)
reduced_precision.defvjp(low_keep, low_pass)
reduced_backward.defvjp(back_keep, back_low)

def matrix_product(left, right):
    return jnp.dot(left, right, precision=lax.Precision.HIGHEST, preferred_element_type=jnp.float32)

def rms_unit(value_heads_out):
    return value_heads_out * lax.rsqrt(lax.optimization_barrier(jnp.mean(value_heads_out * value_heads_out, axis=-1, keepdims=True)) + EPS)

def rotate(value_heads_out, cos_table, sin_table):
    half_dim = value_heads_out.shape[-1] // 2
    lower_half = value_heads_out[..., :half_dim]
    upper_half = value_heads_out[..., half_dim:]
    return jnp.concatenate([lower_half * cos_table - upper_half * sin_table, upper_half * cos_table + lower_half * sin_table], axis=-1)

def block_tables(doc_start):
    starts = doc_start.reshape(-1, TOKENS_PER_SHARD)
    places = jnp.arange(TOKENS_PER_SHARD, dtype=jnp.int32)
    begins = lax.cummax(jnp.where(starts == 1, places[None, :], 0), axis=1)
    offset = (places[None, :] - begins).astype(jnp.float32).reshape(-1)
    frequency = THETA ** (-(jnp.arange(HEAD_SIZE // 2, dtype=jnp.float32) * 2.0 / HEAD_SIZE))
    angles = offset[:, None] * frequency[None, :]
    document_index = jnp.cumsum(starts, axis=1)
    return (jnp.cos(angles)[:, None, :], jnp.sin(angles)[:, None, :], document_index)

def expert_tables(routes):
    block_list = TOKEN_COUNT // TOKENS_PER_SHARD
    per_block = TOKENS_PER_SHARD * TOPK
    chosen = routes.reshape(block_list, per_block)
    onehot = (chosen[:, :, None] == jnp.arange(EXPERTS, dtype=jnp.int32)[None, None, :]).astype(jnp.int32)
    slot_of = lax.optimization_barrier(jnp.sum((jnp.cumsum(onehot, axis=1) - onehot) * onehot, axis=-1))
    places = jnp.arange(block_list, dtype=jnp.int32)[:, None] * MOST + slot_of
    assign = jnp.arange(block_list * per_block, dtype=jnp.int32).reshape(block_list, per_block)
    owners = jnp.full((EXPERTS, block_list * MOST), block_list * per_block, jnp.int32)
    return owners.at[chosen, places].set(assign)

def attention_apply(bundle):
    query_row_matrix, key_row_matrix, value_heads_out, document_index = bundle
    query_group_width = QUERY_HEADS // KEY_VALUE_HEADS
    places = jnp.arange(TOKENS_PER_SHARD, dtype=jnp.int32)
    grouped_heads = query_row_matrix.reshape(TOKENS_PER_SHARD, KEY_VALUE_HEADS, query_group_width, HEAD_SIZE)
    scores = jnp.einsum('qngd,knd->ngqk', grouped_heads, key_row_matrix, precision=lax.Precision.HIGHEST, preferred_element_type=jnp.float32) * HEAD_SIZE ** (-0.5)
    scores = reduced_backward(scores)
    allowed = (document_index[:, None] == document_index[None, :]) & (places[:, None] >= places[None, :])
    scores = jnp.where(allowed, scores, NEG)
    row_peak = lax.optimization_barrier(jnp.max(scores, axis=-1, keepdims=True))
    weights = jnp.exp(scores - row_peak)
    probs_low = reduced_precision(weights / lax.optimization_barrier(jnp.sum(weights, axis=-1, keepdims=True)))
    mixed_token_rows = jnp.einsum('ngqk,knd->qngd', probs_low, value_heads_out, precision=lax.Precision.HIGHEST, preferred_element_type=jnp.float32)
    return mixed_token_rows.reshape(TOKENS_PER_SHARD, QUERY_HEADS * HEAD_SIZE)

def reference(tokens, attn_gain, moe_gain, query_gain, key_gain, query_weight, key_weight, value_matrix, output_weight, gate_proj, up_proj, down_proj, gate_weights, routes, doc_start, cotangent):
    cos_table, sin_table, document_index = block_tables(doc_start)
    owners = expert_tables(routes)
    block_list = TOKEN_COUNT // TOKENS_PER_SHARD
    half_width = FFE // N_TENSOR

    def forward(inputs, gain_attn, gain_moe, gain_query, gain_key, weight_query, key_projection, value_projection, weight_output, gate_mat, up_mat, down_mat, gates):
        normalized_input = reduced_precision(rms_unit(inputs) * gain_attn)
        query_raw = reduced_backward(matrix_product(normalized_input, weight_query)).reshape(TOKEN_COUNT, QUERY_HEADS, HEAD_SIZE)
        key_unrotated = reduced_backward(matrix_product(normalized_input, key_projection)).reshape(TOKEN_COUNT, KEY_VALUE_HEADS, HEAD_SIZE)
        value_heads_out = reduced_precision(reduced_backward(matrix_product(normalized_input, value_projection))).reshape(TOKEN_COUNT, KEY_VALUE_HEADS, HEAD_SIZE)
        query_heads_out = reduced_precision(rotate(rms_unit(query_raw) * gain_query, cos_table, sin_table))
        key_row_matrix = reduced_precision(rotate(rms_unit(key_unrotated) * gain_key, cos_table, sin_table))
        mixed_token_rows = lax.map(jax.checkpoint(attention_apply), (query_heads_out.reshape(block_list, TOKENS_PER_SHARD, QUERY_HEADS, HEAD_SIZE), key_row_matrix.reshape(block_list, TOKENS_PER_SHARD, KEY_VALUE_HEADS, HEAD_SIZE), value_heads_out.reshape(block_list, TOKENS_PER_SHARD, KEY_VALUE_HEADS, HEAD_SIZE), document_index))
        mixed_token_rows = reduced_precision(reduced_backward(mixed_token_rows.reshape(TOKEN_COUNT, QUERY_HEADS * HEAD_SIZE)))
        hidden = inputs + reduced_backward(matrix_product(mixed_token_rows, weight_output.T))
        normed_moe = reduced_precision(rms_unit(hidden) * gain_moe)
        padded = jnp.concatenate([normed_moe, jnp.zeros((1, MODEL_WIDTH), jnp.float32)], axis=0)
        gate_pad = jnp.concatenate([gates.reshape(-1), jnp.zeros((1,), jnp.float32)], axis=0)

        def expert(bundle):
            gate_one, up_one, down_one, owner_row = bundle
            picked = padded[owner_row // TOPK]
            running = jnp.zeros((owner_row.shape[0], MODEL_WIDTH), jnp.float32)
            for portion in range(N_TENSOR):
                lower_col = portion * half_width
                entry_rows = reduced_backward(picked)
                gate_value = reduced_backward(matrix_product(entry_rows, gate_one[:, lower_col:lower_col + half_width]))
                up_value = reduced_backward(matrix_product(entry_rows, up_one[:, lower_col:lower_col + half_width]))
                hidden_act = reduced_precision(jax.nn.silu(gate_value) * up_value)
                running = running + reduced_precision(reduced_backward(matrix_product(hidden_act, down_one[lower_col:lower_col + half_width, :])))
            return gate_pad[owner_row][:, None] * running
        spread = lax.map(jax.checkpoint(expert), (gate_mat, up_mat, down_mat, owners))
        moe_total = jnp.zeros((TOKEN_COUNT + 1, MODEL_WIDTH), jnp.float32).at[(owners // TOPK).reshape(-1)].add(spread.reshape(-1, MODEL_WIDTH))
        return hidden + moe_total[:TOKEN_COUNT]
    floats = tuple((source.astype(jnp.float32) for source in (tokens, attn_gain, moe_gain, query_gain, key_gain, query_weight, key_weight, value_matrix, output_weight, gate_proj, up_proj, down_proj, gate_weights)))
    result, pullback = jax.vjp(forward, *floats)
    gradients = pullback(cotangent.astype(jnp.float32))
    return (result.astype(jnp.bfloat16), gradients[0], gradients[5], gradients[6], gradients[7], gradients[8], gradients[1], gradients[2], gradients[3], gradients[4], gradients[9], gradients[10], gradients[11], gradients[12])
```

```python
import functools
import jax
import jax.numpy as jnp
from jax import lax
from jax.experimental import pallas as pl
from jax.experimental.pallas import tpu as pltpu
from jax.sharding import PartitionSpec as P

HEAD_SIZE = 128


EPS = 1e-06
NEG = -1e30
THETA = 1000000.0


def rms_parts(value_heads_out):
    factor = lax.rsqrt(jnp.mean(value_heads_out * value_heads_out, axis=-1, keepdims=True) + EPS)
    return (value_heads_out * factor, factor)


def norm_back(grad_unit, unit_value, factor):
    return factor * (
        grad_unit - unit_value * jnp.mean(grad_unit * unit_value, axis=-1, keepdims=True)
    )


def rotate(value_heads_out, cos_table, sin_table):
    half_dim = value_heads_out.shape[-1] // 2
    lower_half = value_heads_out[..., :half_dim]
    upper_half = value_heads_out[..., half_dim:]
    return jnp.concatenate(
        [
            lower_half * cos_table - upper_half * sin_table,
            upper_half * cos_table + lower_half * sin_table,
        ],
        axis=-1,
    )


def doc_tables(doc_start):
    row_count = doc_start.shape[0]
    places = jnp.arange(row_count, dtype=jnp.int32)
    begins = lax.cummax(jnp.where(doc_start == 1, places, 0), axis=0)
    offset = (places - begins).astype(jnp.float32)
    frequency = THETA ** (-(jnp.arange(HEAD_SIZE // 2, dtype=jnp.float32) * 2.0 / HEAD_SIZE))
    angles = offset[:, None] * frequency[None, :]
    document_index = jnp.cumsum(doc_start)
    allowed = (document_index[:, None] == document_index[None, :]) & (
        places[:, None] >= places[None, :]
    )
    return (jnp.cos(angles)[:, None, :], jnp.sin(angles)[:, None, :], allowed)


def scores_of(grouped_heads, keys_low, allowed):
    scaled = jnp.einsum(
        "qngd,knd->ngqk", grouped_heads, keys_low, preferred_element_type=jnp.float32
    ) * HEAD_SIZE ** (-0.5)
    return jnp.where(allowed, scaled, NEG)


def to_owners(fetcher, experts, capacity):
    picked = fetcher(jnp.arange(experts * capacity, dtype=jnp.int32)).reshape(experts, capacity, -1)
    arrived = lax.all_to_all(picked, "expert", split_axis=0, concat_axis=0, tiled=True)
    return arrived


def to_sources(expert_rows, places_sent):
    width = expert_rows.shape[-1]
    returned = lax.all_to_all(expert_rows, "expert", split_axis=0, concat_axis=0, tiled=True)
    return returned.reshape(-1, width)[places_sent].astype(jnp.float32)


def local(
    tokens,
    attn_gain,
    moe_gain,
    query_gain,
    key_gain,
    query_weight,
    key_weight,
    value_matrix,
    output_weight,
    gate_proj,
    up_proj,
    down_proj,
    gate_weights,
    routes,
    doc_start,
    cotangent,
):
    gathered = (
        lax.all_gather(query_weight, "expert", axis=0, tiled=True),
        lax.all_gather(key_weight, "expert", axis=0, tiled=True),
        lax.all_gather(value_matrix, "expert", axis=0, tiled=True),
        lax.all_gather(output_weight, "expert", axis=0, tiled=True),
        lax.all_gather(attn_gain, "expert", axis=0, tiled=True),
        lax.all_gather(moe_gain, "expert", axis=0, tiled=True),
        lax.all_gather(query_gain, "expert", axis=0, tiled=True),
        lax.all_gather(key_gain, "expert", axis=0, tiled=True),
    )
    full_query, full_key, full_value, full_output = (
        gathered[0],
        gathered[1],
        gathered[2],
        gathered[3],
    )
    gain_attn = gathered[4].astype(jnp.float32)
    gain_moe = gathered[5].astype(jnp.float32)
    gain_query = gathered[6].astype(jnp.float32)
    gain_key = gathered[7].astype(jnp.float32)
    cos_table, sin_table, allowed = doc_tables(doc_start)
    tok_rows = tokens.shape[0]
    heads_here = full_query.shape[1] // HEAD_SIZE
    kv_here = full_key.shape[1] // HEAD_SIZE
    query_group_width = heads_here // kv_here
    inputs = tokens.astype(jnp.float32)
    unit_attn, factor_attn = rms_parts(inputs)
    normalized_input = (unit_attn * gain_attn).astype(jnp.bfloat16)
    query_raw = jnp.dot(normalized_input, full_query, preferred_element_type=jnp.float32).reshape(
        tok_rows, heads_here, HEAD_SIZE
    )
    key_unrotated = jnp.dot(normalized_input, full_key, preferred_element_type=jnp.float32).reshape(
        tok_rows, kv_here, HEAD_SIZE
    )
    values_low = (
        jnp.dot(normalized_input, full_value, preferred_element_type=jnp.float32)
        .astype(jnp.bfloat16)
        .reshape(tok_rows, kv_here, HEAD_SIZE)
    )
    query_unit, query_factor = rms_parts(query_raw)
    key_unit, key_factor = rms_parts(key_unrotated)
    queries_low = rotate(query_unit * gain_query, cos_table, sin_table).astype(jnp.bfloat16)
    keys_low = rotate(key_unit * gain_key, cos_table, sin_table).astype(jnp.bfloat16)
    grouped_heads = queries_low.reshape(tok_rows, kv_here, query_group_width, HEAD_SIZE)
    scores = scores_of(grouped_heads, keys_low, allowed)
    row_peak = jnp.max(scores, axis=-1, keepdims=True)
    weights = jnp.exp(scores - row_peak)
    totals = jnp.sum(weights, axis=-1, keepdims=True)
    probs_low = (weights / totals).astype(jnp.bfloat16)
    log_total = row_peak + jnp.log(totals)
    mixed_low = (
        jnp.einsum("ngqk,knd->qngd", probs_low, values_low, preferred_element_type=jnp.float32)
        .reshape(tok_rows, heads_here * HEAD_SIZE)
        .astype(jnp.bfloat16)
    )
    attn_part = jnp.einsum("th,dh->td", mixed_low, full_output, preferred_element_type=jnp.float32)
    hidden = inputs + lax.psum(attn_part, "tensor")
    unit_moe, factor_moe = rms_parts(hidden)
    normed_moe = (unit_moe * gain_moe).astype(jnp.bfloat16)
    n_devices = lax.axis_size("expert")
    local_experts = gate_proj.shape[0]
    experts = n_devices * local_experts
    top_count = routes.shape[1]
    assigned = tok_rows * top_count
    capacity = assigned * 5 // (4 * experts)
    chosen = routes.reshape(assigned)
    onehot = (chosen[:, None] == jnp.arange(experts, dtype=jnp.int32)[None, :]).astype(jnp.int32)
    slot_of = jnp.sum((jnp.cumsum(onehot, axis=0) - onehot) * onehot, axis=1)
    places_sent = chosen * capacity + slot_of
    slot_owner = (
        jnp.full((experts * capacity,), assigned, jnp.int32)
        .at[places_sent]
        .set(jnp.arange(assigned, dtype=jnp.int32))
    )
    normed_pad = jnp.concatenate(
        [normed_moe, jnp.zeros((1, normed_moe.shape[1]), jnp.bfloat16)], axis=0
    )

    def fetch_rows(slot_ids):
        return normed_pad[slot_owner[slot_ids] // top_count]

    arrived = to_owners(fetch_rows, experts, capacity).reshape(
        n_devices, local_experts, capacity, -1
    )
    gate_value = jnp.einsum(
        "sled,ldf->slef", arrived, gate_proj, preferred_element_type=jnp.float32
    )
    up_value = jnp.einsum("sled,ldf->slef", arrived, up_proj, preferred_element_type=jnp.float32)
    hidden_act = (jax.nn.silu(gate_value) * up_value).astype(jnp.bfloat16)
    out_rows = jnp.einsum(
        "slef,lfd->sled", hidden_act, down_proj, preferred_element_type=jnp.float32
    ).astype(jnp.bfloat16)
    per_choice = to_sources(out_rows.reshape(experts, capacity, -1), places_sent).reshape(
        tok_rows, top_count, -1
    )
    moe_part = jnp.sum(gate_weights[:, :, None] * per_choice, axis=1)
    moe_out = lax.psum(moe_part.astype(jnp.bfloat16), "tensor").astype(jnp.float32)
    block_out = (hidden + moe_out).astype(jnp.bfloat16)
    upstream = cotangent.astype(jnp.float32)
    gate_part = jnp.sum(per_choice * upstream[:, None, :], axis=-1)
    cot_pad = jnp.concatenate([cotangent, jnp.zeros((1, cotangent.shape[1]), jnp.bfloat16)], axis=0)
    weight_pad = jnp.concatenate(
        [gate_weights.reshape(assigned), jnp.zeros((1,), jnp.float32)], axis=0
    )

    def fetch_grads(slot_ids):
        chosen_slot = slot_owner[slot_ids]
        return (
            weight_pad[chosen_slot][:, None] * cot_pad[chosen_slot // top_count].astype(jnp.float32)
        ).astype(jnp.bfloat16)

    grad_rows = to_owners(fetch_grads, experts, capacity).reshape(
        n_devices, local_experts, capacity, -1
    )
    grad_act = jnp.einsum(
        "sled,lfd->slef", grad_rows, down_proj, preferred_element_type=jnp.float32
    )
    grad_down = jnp.einsum(
        "slef,sled->lfd", hidden_act, grad_rows, preferred_element_type=jnp.float32
    )
    sigmoid_gate = jax.nn.sigmoid(gate_value)
    grad_up_low = (grad_act * gate_value * sigmoid_gate).astype(jnp.bfloat16)
    grad_gate_low = (
        grad_act * up_value * sigmoid_gate * (1.0 + gate_value * (1.0 - sigmoid_gate))
    ).astype(jnp.bfloat16)
    grad_gate_w = jnp.einsum(
        "sled,slef->ldf", arrived, grad_gate_low, preferred_element_type=jnp.float32
    )
    grad_up_w = jnp.einsum(
        "sled,slef->ldf", arrived, grad_up_low, preferred_element_type=jnp.float32
    )
    grad_in = jnp.einsum(
        "slef,ldf->sled", grad_gate_low, gate_proj, preferred_element_type=jnp.float32
    )
    grad_in = (
        grad_in
        + jnp.einsum("slef,ldf->sled", grad_up_low, up_proj, preferred_element_type=jnp.float32)
    ).astype(jnp.bfloat16)
    grad_choice = to_sources(grad_in.reshape(experts, capacity, -1), places_sent).reshape(
        tok_rows, top_count, -1
    )
    grad_moe_part = jnp.sum(grad_choice, axis=1)
    grad_normed_moe, grad_gates = lax.psum((grad_moe_part, gate_part), "tensor")
    grad_moe_gain = jnp.sum(grad_normed_moe * unit_moe, axis=0)
    grad_hidden = upstream + norm_back(grad_normed_moe * gain_moe, unit_moe, factor_moe)
    grad_attn_low = grad_hidden.astype(jnp.bfloat16)
    back_query, back_key, back_value, back_output = (full_query, full_key, full_value, full_output)
    grad_mixed = jnp.einsum(
        "td,dh->th", grad_attn_low, back_output, preferred_element_type=jnp.float32
    )
    grad_mixed_low = grad_mixed.astype(jnp.bfloat16).reshape(
        tok_rows, kv_here, query_group_width, HEAD_SIZE
    )
    grad_output_w = jnp.einsum(
        "td,th->dh", grad_attn_low, mixed_low, preferred_element_type=jnp.float32
    )
    scores = scores_of(grouped_heads, keys_low, allowed)
    prob_full = jnp.exp(scores - log_total)
    grad_probs = jnp.einsum(
        "qngd,knd->ngqk", grad_mixed_low, values_low, preferred_element_type=jnp.float32
    )
    grad_values = jnp.einsum(
        "ngqk,qngd->knd",
        prob_full.astype(jnp.bfloat16),
        grad_mixed_low,
        preferred_element_type=jnp.float32,
    ).astype(jnp.bfloat16)
    row_delta = jnp.sum(prob_full * grad_probs, axis=-1, keepdims=True)
    grad_scores = (prob_full * (grad_probs - row_delta)).astype(jnp.bfloat16)
    score_scale = HEAD_SIZE ** (-0.5)
    grad_queries = (
        jnp.einsum(
            "ngqk,knd->qngd", grad_scores, keys_low, preferred_element_type=jnp.float32
        ).reshape(tok_rows, heads_here, HEAD_SIZE)
        * score_scale
    )
    grad_keys = (
        jnp.einsum("ngqk,qngd->knd", grad_scores, grouped_heads, preferred_element_type=jnp.float32)
        * score_scale
    )
    grad_qhead = rotate(grad_queries, cos_table, -sin_table)
    grad_khead = rotate(grad_keys, cos_table, -sin_table)
    query_gain_part = jnp.sum(grad_qhead * query_unit, axis=(0, 1))
    key_gain_part = jnp.sum(grad_khead * key_unit, axis=(0, 1))
    grad_query_low = (
        norm_back(grad_qhead * gain_query, query_unit, query_factor)
        .astype(jnp.bfloat16)
        .reshape(tok_rows, heads_here * HEAD_SIZE)
    )
    grad_key_low = (
        norm_back(grad_khead * gain_key, key_unit, key_factor)
        .astype(jnp.bfloat16)
        .reshape(tok_rows, kv_here * HEAD_SIZE)
    )
    grad_value_low = grad_values.reshape(tok_rows, kv_here * HEAD_SIZE)
    grad_normed_part = jnp.einsum(
        "th,dh->td", grad_query_low, back_query, preferred_element_type=jnp.float32
    )
    grad_normed_part = grad_normed_part + jnp.einsum(
        "th,dh->td", grad_key_low, back_key, preferred_element_type=jnp.float32
    )
    grad_normed_part = grad_normed_part + jnp.einsum(
        "th,dh->td", grad_value_low, back_value, preferred_element_type=jnp.float32
    )
    grad_query_w = jnp.einsum(
        "td,th->dh", normalized_input, grad_query_low, preferred_element_type=jnp.float32
    )
    grad_key_w = jnp.einsum(
        "td,th->dh", normalized_input, grad_key_low, preferred_element_type=jnp.float32
    )
    grad_value_w = jnp.einsum(
        "td,th->dh", normalized_input, grad_value_low, preferred_element_type=jnp.float32
    )
    grad_normed, query_gain_sum, key_gain_sum = (
        lax.psum(grad_normed_part.astype(jnp.bfloat16), "tensor").astype(jnp.float32),
        lax.psum(query_gain_part.astype(jnp.bfloat16), "tensor").astype(jnp.float32),
        lax.psum(key_gain_part.astype(jnp.bfloat16), "tensor").astype(jnp.float32),
    )
    grad_attn_gain_part = jnp.sum(grad_normed * unit_attn, axis=0)
    grad_tokens = grad_hidden + norm_back(grad_normed * gain_attn, unit_attn, factor_attn)
    shares = (
        lax.psum_scatter(grad_query_w, "expert", scatter_dimension=0, tiled=True),
        lax.psum_scatter(grad_key_w, "expert", scatter_dimension=0, tiled=True),
        lax.psum_scatter(grad_value_w, "expert", scatter_dimension=0, tiled=True),
        lax.psum_scatter(grad_output_w, "expert", scatter_dimension=0, tiled=True),
        lax.psum_scatter(grad_attn_gain_part, "expert", scatter_dimension=0, tiled=True),
        lax.psum_scatter(grad_moe_gain, "expert", scatter_dimension=0, tiled=True),
        lax.psum_scatter(query_gain_sum, "expert", scatter_dimension=0, tiled=True),
        lax.psum_scatter(key_gain_sum, "expert", scatter_dimension=0, tiled=True),
    )
    return (
        block_out,
        grad_tokens,
        shares[0],
        shares[1],
        shares[2],
        shares[3],
        shares[4],
        shares[5],
        shares[6],
        shares[7],
        grad_gate_w,
        grad_up_w,
        grad_down,
        grad_gates,
    )


MESH = pl.DeviceIdType.MESH
ZS, YS, XS = 4, 2, 2

def place():
    e = lax.axis_index("expert"); c = lax.axis_index("tensor")
    return e // 4, (e // 2) % 2, e % 2, c

def ident(z, y, x, c):
    return (z * 4 + y * 2 + x, c)

def greet(share):
    z, y, x, c = place()
    bar = pltpu.get_barrier_semaphore()
    def hello(dev):
        pl.semaphore_signal(bar, inc=1, device_id=dev, device_id_type=MESH)
    hello(ident(z, y, 1 - x, c))
    hello(ident(z, 1 - y, x, c))
    n = 2
    if share:
        hello(ident(z, y, x, 1 - c)); n = 3
    pl.when(z > 0)(lambda: hello(ident(z - 1, y, x, c)))
    pl.when(z < ZS - 1)(lambda: hello(ident(z + 1, y, x, c)))
    pl.semaphore_wait(bar, n + (z > 0).astype(jnp.int32) + (z < ZS - 1).astype(jnp.int32))

def gather_kernel(n, share, *refs):
    ins, outs = refs[:n], refs[n:2 * n]
    stage = refs[2 * n:3 * n]
    ss, rs, ls = refs[3 * n:]
    z, y, x, c = place()
    greet(share)
    rows = [(r.shape[0] // 2 if share else r.shape[0]) for r in ins]
    full = [r.shape[0] for r in ins]
    def start(a, b, part):
        base = (z * 0 + b) * full[a]
        if share:
            base = base + c * rows[a]
        half = rows[a] // 2
        if part == "w":
            return pl.ds(pl.multiple_of(base, 16), rows[a])
        return pl.ds(pl.multiple_of(base + (0 if part == "p" else half), 16), half)
    def src_own(a, part):
        half = rows[a] // 2
        base = c * rows[a] if share else 0
        if part == "w":
            return ins[a].at[pl.ds(base, rows[a]), :]
        off = 0 if part == "p" else half
        return ins[a].at[pl.ds(base + off, half), :]
    keys = {}
    def num(k):
        return keys.setdefault(k, len(keys))
    def cp(k, a, b, part, dev, own=False):
        i = num(k)
        dst = outs[a].at[start(a, b, part), :]
        src = src_own(a, part) if own else dst
        return pltpu.make_async_remote_copy(src_ref=src, dst_ref=dst, send_sem=ss.at[i, a], recv_sem=rs.at[i, a],
                                            device_id=dev, device_id_type=MESH)
    def each(f):
        for a in range(n):
            f(a)
    xn, yn, zu, zd, sib = ident(z, y, 1 - x, c), ident(z, 1 - y, x, c), ident(z + 1, y, x, c), ident(z - 1, y, x, c), ident(z, y, x, 1 - c)
    def bid(s, yy, xx):
        return s * 4 + yy * 2 + xx
    sends = []
    me = bid(z, y, x)
    locs = []
    def own_in(a):
        return pltpu.make_async_copy(ins[a], stage[a], ls.at[a, 0])
    def own_out(a):
        return pltpu.make_async_copy(stage[a], outs[a].at[pl.ds(pl.multiple_of(me * full[a], 16), full[a]), :], ls.at[a, 1])
    def send(cond, k, b, part, dev, own=False):
        def go():
            each(lambda a: cp(k, a, b, part, dev, own).start())
        if cond is None: go()
        else: pl.when(cond)(go)
        sends.append((cond, k, b, part, dev, own))
    def recv(cond, k, b, part, dev):
        def go():
            each(lambda a: cp(k, a, b, part, dev).wait_recv())
        if cond is None: go()
        else: pl.when(cond)(go)
    send(z < 3, ("u", 0), me, "w", zu, True)
    send(z > 0, ("d", 0), me, "w", zd, True)
    slots = [(0, 0)] + [(d, sg) for d in (1, 2, 3) for sg in (-1, 1)]
    def cond_of(d, sg):
        if d == 0: return None
        return (z - d >= 0) if sg < 0 else (z + d <= 3)
    def A(d, sg):
        s = z + sg * d; cnd = cond_of(d, sg); own = d == 0
        b = bid(s, y, x)
        send(cnd, ("xP", d, sg), b, "p", xn, own)
        send(cnd, ("yQ", d, sg), b, "q", yn, own)
        send(cnd, ("xQ", d, sg), b, "q", xn, own)
        send(cnd, ("yP", d, sg), b, "p", yn, own)
        if share and not own:
            send(cnd, ("s0", d, sg), b, "w", sib)
    def B(d, sg):
        s = z + sg * d; cnd = cond_of(d, sg)
        recv(cnd, ("xP", d, sg), bid(s, y, 1 - x), "p", xn)
        send(cnd, ("yPr", d, sg), bid(s, y, 1 - x), "p", yn)
        recv(cnd, ("yQ", d, sg), bid(s, 1 - y, x), "q", yn)
        send(cnd, ("xQr", d, sg), bid(s, 1 - y, x), "q", xn)
    def C(d, sg):
        s = z + sg * d; cnd = cond_of(d, sg)
        recv(cnd, ("xQ", d, sg), bid(s, y, 1 - x), "q", xn)
        if share: send(cnd, ("s1", d, sg), bid(s, y, 1 - x), "w", sib)
        recv(cnd, ("yP", d, sg), bid(s, 1 - y, x), "p", yn)
        if share: send(cnd, ("s2", d, sg), bid(s, 1 - y, x), "w", sib)
        recv(cnd, ("yPr", d, sg), bid(s, 1 - y, 1 - x), "p", yn)
        recv(cnd, ("xQr", d, sg), bid(s, 1 - y, 1 - x), "q", xn)
        if share: send(cnd, ("s3", d, sg), bid(s, 1 - y, 1 - x), "w", sib)
    A(0, 0)
    each(lambda a: own_in(a).start())
    each(lambda a: own_in(a).wait())
    each(lambda a: own_out(a).start())
    B(0, 0)
    prev = [(0, 0)]
    for d in (1, 2, 3):
        recv(z - d >= 0, ("u", d - 1), bid(z - d, y, x), "w", zd)
        if d < 3:
            send((z - d >= 0) & (z < 3), ("u", d), bid(z - d, y, x), "w", zu)
        A(d, -1)
        recv(z + d <= 3, ("d", d - 1), bid(z + d, y, x), "w", zu)
        if d < 3:
            send((z + d <= 3) & (z > 0), ("d", d), bid(z + d, y, x), "w", zd)
        A(d, 1)
        B(d, -1); B(d, 1)
        for p in prev: C(*p)
        prev = [(d, -1), (d, 1)]
    for p in prev: C(*p)
    each(lambda a: own_out(a).wait())
    if share:
        for d, sg in slots:
            s = z + sg * d; cnd = cond_of(d, sg)
            def sibwait(k, b):
                def go():
                    for a in range(n):
                        i = num(k)
                        r = outs[a].at[pl.ds(pl.multiple_of(b * full[a] + (1 - c) * rows[a], 16), rows[a]), :]
                        pltpu.make_async_remote_copy(src_ref=r, dst_ref=r, send_sem=ss.at[i, a], recv_sem=rs.at[i, a], device_id=sib, device_id_type=MESH).wait_recv()
                if cnd is None: go()
                else: pl.when(cnd)(go)
            if d: sibwait(("s0", d, sg), bid(s, y, x))
            sibwait(("s1", d, sg), bid(s, y, 1 - x))
            sibwait(("s2", d, sg), bid(s, 1 - y, x))
            sibwait(("s3", d, sg), bid(s, 1 - y, 1 - x))
    for cond, k, b, part, dev, own in sends:
        def go():
            each(lambda a: cp(k, a, b, part, dev, own).wait_send())
        if cond is None: go()
        else: pl.when(cond)(go)
    assert len(keys) <= NKEYS, len(keys)

NKEYS = 80
def all_gather_blocks(arrays, cid, share=False):
    n = len(arrays)
    anyspec = pl.BlockSpec(memory_space=pltpu.HBM)
    return pl.pallas_call(
        functools.partial(gather_kernel, n, share),
        out_shape=[jax.ShapeDtypeStruct((16 * a.shape[0], a.shape[1]), a.dtype) for a in arrays],
        in_specs=[anyspec] * n, out_specs=[anyspec] * n,
        scratch_shapes=[pltpu.VMEM(a.shape, a.dtype) for a in arrays] + [
            pltpu.SemaphoreType.DMA((NKEYS, n)), pltpu.SemaphoreType.DMA((NKEYS, n)), pltpu.SemaphoreType.DMA((n, 2))],
        compiler_params=pltpu.CompilerParams(collective_id=cid, has_side_effects=True),
        name="gather_blocks",
    )(*arrays)


SLOTS = [(3, -1), (3, 1), (2, -1), (2, 1), (1, -1), (1, 1), (0, 0)]
CH = 32

def scatter_kernel(part, out, A, SR, RP, RP2, RQ, RQ2, ZU, ZD, ls, ss, rs):
    z, y, x, c = place()
    rows = A.shape[1]; half = rows // 2
    greet(True)
    xn, yn, zu, zd, sib = ident(z, y, 1 - x, c), ident(z, 1 - y, x, c), ident(z + 1, y, x, c), ident(z - 1, y, x, c), ident(z, y, x, 1 - c)
    keys = {}
    def num(k): return keys.setdefault(k, len(keys))
    def cond_of(d, sg):
        if d == 0: return None
        return (z - d >= 0) if sg < 0 else (z + d <= 3)
    def guard(cnd, go):
        if cnd is None: go()
        else: pl.when(cnd)(go)
    sent = []
    def rc(k, src, dst, dev):
        i = num(k)
        return pltpu.make_async_remote_copy(src_ref=src, dst_ref=dst, send_sem=ss.at[i], recv_sem=rs.at[i], device_id=dev, device_id_type=MESH)
    def send(cnd, k, src, dst, dev):
        guard(cnd, lambda: rc(k, src, dst, dev).start())
        sent.append((cnd, k, src, dst, dev))
    def recv(cnd, k, dst, dev):
        guard(cnd, lambda: rc(k, dst, dst, dev).wait_recv())
    def blocks(s):
        b = s * 4
        return b + y * 2 + x, b + y * 2 + 1 - x, b + (1 - y) * 2 + x, b + (1 - y) * 2 + 1 - x
    Ph, Qh = pl.ds(0, half), pl.ds(half, half)
    def part_at(b, cc):
        return part.at[pl.ds(pl.multiple_of(b * 2 * rows + cc * rows, 16), rows), :]
    def load(b):
        return pltpu.make_async_copy(part_at(b, c), A.at[b], ls.at[b])
    for d, sg in SLOTS:
        cnd = cond_of(d, sg); s = z + sg * d
        for q, b in enumerate(blocks(s)):
            guard(cnd, lambda: load(b).start())
            send(cnd, ("sib", d, sg, q), part_at(b, 1 - c), SR.at[b], sib)
    def sum_into(dst, row0, terms, n=half):
        def step(i, _):
            r = pl.ds(row0 + i * CH, CH)
            acc = dst[r, :].astype(jnp.float32)
            for t, off in terms:
                acc = acc + t[pl.ds(off + i * CH, CH), :].astype(jnp.float32)
            dst[r, :] = acc.astype(dst.dtype)
            return 0
        lax.fori_loop(0, n // CH, step, 0)
    def S1(i):
        d, sg = SLOTS[i]; cnd = cond_of(d, sg); s = z + sg * d
        m, xx, yy, dd = blocks(s)
        def go():
            for q, b in enumerate((m, xx, yy, dd)):
                load(b).wait()
                rc(("sib", d, sg, q), SR.at[b], SR.at[b], sib).wait_recv()
            sum_into(A.at[dd], 0, [(SR.at[dd], 0)], rows)
        guard(cnd, go)
        send(cnd, ("yd", i), A.at[dd, Ph, :], RP.at[s, 1], yn)
        send(cnd, ("xd", i), A.at[dd, Qh, :], RQ.at[s, 1], xn)
        guard(cnd, lambda: (sum_into(A.at[yy], 0, [(SR.at[yy], 0)]), sum_into(A.at[xx], half, [(SR.at[xx], half)]))and None)
        send(cnd, ("yy", i), A.at[yy, Ph, :], RP.at[s, 0], yn)
        send(cnd, ("xx", i), A.at[xx, Qh, :], RQ.at[s, 0], xn)
    def S2(i):
        d, sg = SLOTS[i]; cnd = cond_of(d, sg); s = z + sg * d
        m, xx, yy, dd = blocks(s)
        recv(cnd, ("yd", i), RP.at[s, 1], yn)
        guard(cnd, lambda: sum_into(A.at[xx], 0, [(SR.at[xx], 0), (RP.at[s, 1], 0)]))
        send(cnd, ("x2", i), A.at[xx, Ph, :], RP2.at[s], xn)
        recv(cnd, ("xd", i), RQ.at[s, 1], xn)
        guard(cnd, lambda: sum_into(A.at[yy], half, [(SR.at[yy], half), (RQ.at[s, 1], 0)]))
        send(cnd, ("y2", i), A.at[yy, Qh, :], RQ2.at[s], yn)
    def S3(i):
        d, sg = SLOTS[i]; cnd = cond_of(d, sg); s = z + sg * d
        m = blocks(s)[0]
        recv(cnd, ("yy", i), RP.at[s, 0], yn)
        recv(cnd, ("xx", i), RQ.at[s, 0], xn)
        recv(cnd, ("x2", i), RP2.at[s], xn)
        recv(cnd, ("y2", i), RQ2.at[s], yn)
        base_p = [(SR.at[m], 0), (RP.at[s, 0], 0), (RP2.at[s], 0)]
        base_q = [(SR.at[m], half), (RQ.at[s, 0], 0), (RQ2.at[s], 0)]
        if d:
            back = (z > 0) if sg > 0 else (z < 3)
            Z = ZU if sg > 0 else ZD
            name = "u" if sg > 0 else "d"
            dn, up = (zd, zu) if sg > 0 else (zu, zd)
            has = d <= 2
            def plain():
                sum_into(A.at[m], 0, base_p); sum_into(A.at[m], half, base_q)
            if has:
                recv(cnd & back, (name, d), Z.at[d], dn)
                pl.when(cnd & back)(lambda: (sum_into(A.at[m], 0, base_p + [(Z.at[d], 0)]), sum_into(A.at[m], half, base_q + [(Z.at[d], half)])) and None)
                pl.when(cnd & jnp.logical_not(back))(plain)
            else:
                pl.when(cnd)(plain)
            send(cnd, (name, d - 1), A.at[m], Z.at[d - 1], up)
        else:
            recv(z > 0, ("u", 0), ZU.at[0], zd)
            recv(z < 3, ("d", 0), ZD.at[0], zu)
            lo = jnp.where(z > 0, 1.0, 0.0); hi = jnp.where(z < 3, 1.0, 0.0)
            def emit(row0, terms, flags):
                def step(i, _):
                    acc = A[m, pl.ds(row0 + i * CH, CH), :].astype(jnp.float32)
                    for t, off in terms:
                        acc = acc + t[pl.ds(off + i * CH, CH), :].astype(jnp.float32)
                    if flags[0]: acc = acc + ZU[0, pl.ds(row0 + i * CH, CH), :].astype(jnp.float32)
                    if flags[1]: acc = acc + ZD[0, pl.ds(row0 + i * CH, CH), :].astype(jnp.float32)
                    out[pl.ds(pl.multiple_of(c * rows + row0 + i * CH, CH), CH), :] = acc
                    return 0
                lax.fori_loop(0, half // CH, step, 0)
            for cc, fl in ((z == 0, (False, True)), (z == 3, (True, False)), ((z > 0) & (z < 3), (True, True))):
                @pl.when(cc)
                def _(fl=fl):
                    emit(0, base_p, fl); emit(half, base_q, fl)
            mine = out.at[pl.ds(pl.multiple_of(c * rows, 16), rows), :]
            other = out.at[pl.ds(pl.multiple_of((1 - c) * rows, 16), rows), :]
            send(None, ("fin",), mine, mine, sib)
            recv(None, ("fin",), other, sib)
    n = len(SLOTS)
    for i in range(n + 2):
        if i < n: S1(i)
        if 0 <= i - 1 < n: S2(i - 1)
        if 0 <= i - 2 < n: S3(i - 2)
    for cnd, k, src, dst, dev in sent:
        guard(cnd, lambda: rc(k, src, dst, dev).wait_send())
    assert len(keys) <= NK, len(keys)

NK = 90
def reduce_scatter_rows(part, cid):
    total, width = part.shape
    rows = total // 32
    half = rows // 2
    bf = part.dtype
    return pl.pallas_call(
        scatter_kernel,
        out_shape=jax.ShapeDtypeStruct((2 * rows, width), jnp.float32),
        in_specs=[pl.BlockSpec(memory_space=pltpu.HBM)], out_specs=pl.BlockSpec(memory_space=pltpu.VMEM),
        scratch_shapes=[
            pltpu.VMEM((16, rows, width), bf), pltpu.VMEM((16, rows, width), bf),
            pltpu.VMEM((4, 2, half, width), bf), pltpu.VMEM((4, half, width), bf),
            pltpu.VMEM((4, 2, half, width), bf), pltpu.VMEM((4, half, width), bf),
            pltpu.VMEM((3, rows, width), bf), pltpu.VMEM((3, rows, width), bf),
            pltpu.SemaphoreType.DMA((16,)), pltpu.SemaphoreType.DMA((NK,)), pltpu.SemaphoreType.DMA((NK,))],
        compiler_params=pltpu.CompilerParams(collective_id=cid, has_side_effects=True, vmem_limit_bytes=67043328),
        name="scatter_rows",
    )(part)

def tables(routes_all, weights_all, first, local_experts, capacity):
    n, rows, top = routes_all.shape
    tri = (jnp.arange(rows)[:, None] <= jnp.arange(rows)[None, :]).astype(jnp.bfloat16)
    picks, scale, token_w = [], [], []
    for l in range(local_experts):
        hit = routes_all == (first + l)
        member = jnp.any(hit, axis=-1)
        weight = jnp.sum(jnp.where(hit, weights_all, 0.0), axis=-1)
        rank = jnp.dot(member.astype(jnp.bfloat16), tri, preferred_element_type=jnp.float32).astype(jnp.int32)
        slot = jnp.where(member, rank - 1, -1)
        pick = slot[:, None, :] == jnp.arange(capacity, dtype=jnp.int32)[None, :, None]
        picks.append(pick)
        scale.append(jnp.sum(jnp.where(pick, weight[:, None, :], 0.0), axis=-1, keepdims=True))
    return picks, scale


def local_block(
    tokens, attn_gain, moe_gain, query_gain, key_gain, query_weight, key_weight, value_matrix, output_weight,
    gate_proj, up_proj, down_proj, gate_weights, routes, doc_start, cotangent,
):
    f32, bf16 = jnp.float32, jnp.bfloat16
    tok_rows, width = tokens.shape
    top_count = routes.shape[1]
    n_chips = ZS * YS * XS
    assigned = tok_rows * top_count
    lanes = 128
    list_rows = assigned // lanes
    small = jnp.concatenate(
        [
            attn_gain.astype(f32).reshape(-1, lanes), moe_gain.astype(f32).reshape(-1, lanes),
            jnp.pad(jnp.concatenate([query_gain, key_gain]).astype(f32), (0, lanes - 2 * query_gain.shape[0])).reshape(1, lanes),
            routes.astype(f32).reshape(list_rows, lanes), gate_weights.reshape(list_rows, lanes),
        ], axis=0)
    gain_rows = attn_gain.shape[0] // lanes
    small = jnp.pad(small, ((0, -small.shape[0] % 32), (0, 0)))
    full_query, full_key, full_value, full_output, gathered = all_gather_blocks(
        [query_weight, key_weight, value_matrix, output_weight, small], 1)
    (dy_all,) = all_gather_blocks([cotangent], 2, share=True)
    gathered = gathered.reshape(n_chips, -1, lanes)
    gain_attn = gathered[:, :gain_rows].reshape(-1)
    gain_moe = gathered[:, gain_rows:2 * gain_rows].reshape(-1)
    per = query_gain.shape[0]
    gain_query = gathered[:, 2 * gain_rows, :per].reshape(-1)
    gain_key = gathered[:, 2 * gain_rows, per:2 * per].reshape(-1)
    off = 2 * gain_rows + 1
    routes_all = gathered[:, off:off + list_rows].astype(jnp.int32).reshape(n_chips, tok_rows, top_count)
    weights_all = gathered[:, off + list_rows:off + 2 * list_rows].reshape(n_chips, tok_rows, top_count)

    cos_table, sin_table, allowed = doc_tables(doc_start)
    heads_here = full_query.shape[1] // HEAD_SIZE
    kv_here = full_key.shape[1] // HEAD_SIZE
    query_group_width = heads_here // kv_here
    inputs = tokens.astype(f32)
    unit_attn, factor_attn = rms_parts(inputs)
    normalized_input = (unit_attn * gain_attn).astype(bf16)
    query_raw = jnp.dot(normalized_input, full_query, preferred_element_type=f32).reshape(tok_rows, heads_here, HEAD_SIZE)
    key_unrotated = jnp.dot(normalized_input, full_key, preferred_element_type=f32).reshape(tok_rows, kv_here, HEAD_SIZE)
    values_low = jnp.dot(normalized_input, full_value, preferred_element_type=f32).astype(bf16).reshape(tok_rows, kv_here, HEAD_SIZE)
    query_unit, query_factor = rms_parts(query_raw)
    key_unit, key_factor = rms_parts(key_unrotated)
    queries_low = rotate(query_unit * gain_query, cos_table, sin_table).astype(bf16)
    keys_low = rotate(key_unit * gain_key, cos_table, sin_table).astype(bf16)
    grouped_heads = queries_low.reshape(tok_rows, kv_here, query_group_width, HEAD_SIZE)
    scores = scores_of(grouped_heads, keys_low, allowed)
    row_peak = jnp.max(scores, axis=-1, keepdims=True)
    weights = jnp.exp(scores - row_peak)
    totals = jnp.sum(weights, axis=-1, keepdims=True)
    probs_low = (weights / totals).astype(bf16)
    log_total = row_peak + jnp.log(totals)
    mixed_low = (
        jnp.einsum("ngqk,knd->qngd", probs_low, values_low, preferred_element_type=f32)
        .reshape(tok_rows, heads_here * HEAD_SIZE).astype(bf16))
    attn_part = jnp.einsum("th,dh->td", mixed_low, full_output, preferred_element_type=f32)
    hidden = inputs + lax.psum(attn_part, "tensor")
    unit_moe, factor_moe = rms_parts(hidden)
    normed_moe = (unit_moe * gain_moe).astype(bf16)

    local_experts = gate_proj.shape[0]
    experts = n_chips * local_experts
    capacity = assigned * 5 // (4 * experts)
    chip = lax.axis_index("expert")
    picks, scale = tables(routes_all, weights_all, chip * local_experts, local_experts, capacity)
    (x_all,) = all_gather_blocks([normed_moe], 3, share=True)
    x_all = x_all.reshape(n_chips, tok_rows, width)
    dy_all = dy_all.reshape(n_chips, tok_rows, width)
    y_rows, dx_rows, gates_tok, grads = [], [], [], []
    for l in range(local_experts):
        pick = picks[l].astype(bf16)
        def take(source):
            return jnp.einsum("sjt,std->sjd", pick, source, preferred_element_type=f32)
        w_slot = scale[l].reshape(-1, 1)
        xs = take(x_all).astype(bf16).reshape(-1, width)
        dys = (scale[l] * take(dy_all)).astype(bf16).reshape(-1, width)
        gate_value = jnp.dot(xs, gate_proj[l], preferred_element_type=f32)
        up_value = jnp.dot(xs, up_proj[l], preferred_element_type=f32)
        sigmoid_gate = jax.nn.sigmoid(gate_value)
        act = (gate_value * sigmoid_gate * up_value).astype(bf16)
        y_rows.append((w_slot * jnp.dot(act, down_proj[l], preferred_element_type=f32)).astype(bf16))
        grad_act = jnp.einsum("rd,fd->rf", dys, down_proj[l], preferred_element_type=f32)
        gates_slot = jnp.sum(act.astype(f32) * grad_act, axis=-1, keepdims=True) / jnp.where(w_slot > 0, w_slot, 1.0)
        gates_tok.append(jnp.sum(jnp.where(picks[l], gates_slot.reshape(n_chips, capacity, 1), 0.0), axis=1))
        up_low = (grad_act * gate_value * sigmoid_gate).astype(bf16)
        gate_low = (grad_act * up_value * sigmoid_gate * (1.0 + gate_value * (1.0 - sigmoid_gate))).astype(bf16)
        dx = jnp.einsum("rf,df->rd", gate_low, gate_proj[l], preferred_element_type=f32)
        dx = dx + jnp.einsum("rf,df->rd", up_low, up_proj[l], preferred_element_type=f32)
        dx_rows.append(dx.astype(bf16))
        grads.append((
            jnp.einsum("rd,rf->df", xs, gate_low, preferred_element_type=f32),
            jnp.einsum("rd,rf->df", xs, up_low, preferred_element_type=f32),
            jnp.einsum("rf,rd->fd", act, dys, preferred_element_type=f32)))
    pick_both = jnp.concatenate(picks, axis=1).astype(bf16)
    def put(rows):
        both = jnp.concatenate([r.reshape(n_chips, capacity, width) for r in rows], axis=1)
        return jnp.einsum("sjt,sjd->std", pick_both, both, preferred_element_type=f32).astype(bf16).reshape(-1, width)
    grad_normed_moe = reduce_scatter_rows(put(dx_rows), 4)
    moe_out = reduce_scatter_rows(put(y_rows), 5)
    grad_gate_w, grad_up_w, grad_down = (jnp.stack([g[i] for g in grads]) for i in range(3))
    block_out = (hidden + moe_out).astype(bf16)
    gates_back = lax.all_to_all(jnp.stack(gates_tok, axis=1), "expert", split_axis=0, concat_axis=0, tiled=True)
    gates_back = lax.psum(gates_back, "tensor").reshape(experts, tok_rows)
    grad_gates = jnp.sum(
        jnp.where(routes[:, :, None] == jnp.arange(experts, dtype=jnp.int32), gates_back.T[:, None, :], 0.0), axis=-1)

    upstream = cotangent.astype(f32)
    grad_moe_gain = jnp.sum(grad_normed_moe * unit_moe, axis=0)
    grad_hidden = upstream + norm_back(grad_normed_moe * gain_moe, unit_moe, factor_moe)
    grad_attn_low = grad_hidden.astype(bf16)
    grad_mixed = jnp.einsum("td,dh->th", grad_attn_low, full_output, preferred_element_type=f32)
    grad_mixed_low = grad_mixed.astype(bf16).reshape(tok_rows, kv_here, query_group_width, HEAD_SIZE)
    grad_output_w = jnp.einsum("td,th->dh", grad_attn_low, mixed_low, preferred_element_type=f32)
    scores = scores_of(grouped_heads, keys_low, allowed)
    prob_full = jnp.exp(scores - log_total)
    grad_probs = jnp.einsum("qngd,knd->ngqk", grad_mixed_low, values_low, preferred_element_type=f32)
    grad_values = jnp.einsum(
        "ngqk,qngd->knd", prob_full.astype(bf16), grad_mixed_low, preferred_element_type=f32).astype(bf16)
    row_delta = jnp.sum(prob_full * grad_probs, axis=-1, keepdims=True)
    grad_scores = (prob_full * (grad_probs - row_delta)).astype(bf16)
    score_scale = HEAD_SIZE ** (-0.5)
    grad_queries = (
        jnp.einsum("ngqk,knd->qngd", grad_scores, keys_low, preferred_element_type=f32)
        .reshape(tok_rows, heads_here, HEAD_SIZE) * score_scale)
    grad_keys = jnp.einsum("ngqk,qngd->knd", grad_scores, grouped_heads, preferred_element_type=f32) * score_scale
    grad_qhead = rotate(grad_queries, cos_table, -sin_table)
    grad_khead = rotate(grad_keys, cos_table, -sin_table)
    query_gain_part = jnp.sum(grad_qhead * query_unit, axis=(0, 1))
    key_gain_part = jnp.sum(grad_khead * key_unit, axis=(0, 1))
    grad_query_low = norm_back(grad_qhead * gain_query, query_unit, query_factor).astype(bf16).reshape(tok_rows, -1)
    grad_key_low = norm_back(grad_khead * gain_key, key_unit, key_factor).astype(bf16).reshape(tok_rows, -1)
    grad_value_low = grad_values.reshape(tok_rows, -1)
    grad_normed_part = jnp.einsum("th,dh->td", grad_query_low, full_query, preferred_element_type=f32)
    grad_normed_part = grad_normed_part + jnp.einsum("th,dh->td", grad_key_low, full_key, preferred_element_type=f32)
    grad_normed_part = grad_normed_part + jnp.einsum("th,dh->td", grad_value_low, full_value, preferred_element_type=f32)
    grad_normed = lax.psum(grad_normed_part.astype(bf16), "tensor").astype(f32)
    grad_attn_gain_part = jnp.sum(grad_normed * unit_attn, axis=0)
    grad_tokens = grad_hidden + norm_back(grad_normed * gain_attn, unit_attn, factor_attn)

    grad_query_w = jnp.einsum("td,th->dh", normalized_input, grad_query_low, preferred_element_type=f32)
    grad_key_w = jnp.einsum("td,th->dh", normalized_input, grad_key_low, preferred_element_type=f32)
    grad_value_w = jnp.einsum("td,th->dh", normalized_input, grad_value_low, preferred_element_type=f32)
    shares = tuple(
        lax.psum_scatter(v, "expert", scatter_dimension=0, tiled=True)
        for v in (grad_query_w, grad_key_w, grad_value_w, grad_output_w))
    gains = jnp.concatenate([grad_attn_gain_part, grad_moe_gain, query_gain_part, key_gain_part])
    head_gains = lax.psum(gains[2 * width:], ("expert", "tensor"))
    model_gains = lax.psum(gains[:2 * width], "expert")
    def own(v):
        size = v.shape[0] // n_chips
        return lax.dynamic_slice_in_dim(v, chip * size, size, 0)
    return (
        block_out, grad_tokens, *shares,
        own(model_gains[:width]), own(model_gains[width:]), own(head_gains[:HEAD_SIZE]), own(head_gains[HEAD_SIZE:]),
        grad_gate_w, grad_up_w, grad_down, grad_gates,
    )


def solution(mesh):
    wide = mesh.shape["expert"] == ZS * YS * XS and mesh.shape["tensor"] == 2
    return jax.shard_map(
        local_block if wide else local,
        mesh=mesh,
        in_specs=(
            P("expert", None),
            P("expert"),
            P("expert"),
            P("expert"),
            P("expert"),
            P("expert", "tensor"),
            P("expert", "tensor"),
            P("expert", "tensor"),
            P("expert", "tensor"),
            P("expert", None, "tensor"),
            P("expert", None, "tensor"),
            P("expert", "tensor", None),
            P("expert", None),
            P("expert", None),
            P("expert"),
            P("expert", None),
        ),
        out_specs=(
            P("expert", None),
            P("expert", None),
            P("expert", "tensor"),
            P("expert", "tensor"),
            P("expert", "tensor"),
            P("expert", "tensor"),
            P("expert"),
            P("expert"),
            P("expert"),
            P("expert"),
            P("expert", None, "tensor"),
            P("expert", None, "tensor"),
            P("expert", "tensor", None),
            P("expert", None),
        ),
        check_vma=False,
    )
```

```python
import functools
import jax
import jax.numpy as jnp
from jax import lax
from jax.experimental import pallas as pl
from jax.experimental.pallas import tpu as pltpu
from jax.sharding import PartitionSpec as P

NAME_D = 'd'
NAME_EXPERT = 'expert'
NAME_FIN = 'fin'
NAME_GATHER_BLOCKS = 'gather_blocks'
NAME_NGQK_KND_QNGD = 'ngqk,knd->qngd'
NAME_NGQK_QNGD_KND = 'ngqk,qngd->knd'
NAME_P = 'p'
NAME_Q = 'q'
NAME_QNGD_KND_NGQK = 'qngd,knd->ngqk'
NAME_RD_FD_RF = 'rd,fd->rf'
NAME_RD_RF_DF = 'rd,rf->df'
NAME_RF_DF_RD = 'rf,df->rd'
NAME_RF_RD_FD = 'rf,rd->fd'
NAME_S0 = 's0'
NAME_S1 = 's1'
NAME_S2 = 's2'
NAME_S3 = 's3'
NAME_SCATTER_GRADS = 'scatter_grads'
NAME_SCATTER_ROWS = 'scatter_rows'
NAME_SIB = 'sib'
NAME_SJT_SJD_STD = 'sjt,sjd->std'
NAME_SJT_STD_SJD = 'sjt,std->sjd'
NAME_SLED_LDF_SLEF = 'sled,ldf->slef'
NAME_SLED_LFD_SLEF = 'sled,lfd->slef'
NAME_SLED_SLEF_LDF = 'sled,slef->ldf'
NAME_SLEF_LDF_SLED = 'slef,ldf->sled'
NAME_SLEF_LFD_SLED = 'slef,lfd->sled'
NAME_SLEF_SLED_LFD = 'slef,sled->lfd'
NAME_TD_DH_TH = 'td,dh->th'
NAME_TD_TH_DH = 'td,th->dh'
NAME_TENSOR = 'tensor'
NAME_TH_DH_TD = 'th,dh->td'
NAME_U = 'u'
NAME_W = 'w'
NAME_X2 = 'x2'
NAME_XP = 'xP'
NAME_XQ = 'xQ'
NAME_XQR = 'xQr'
NAME_XD = 'xd'
NAME_XX = 'xx'
NAME_Y2 = 'y2'
NAME_YP = 'yP'
NAME_YPR = 'yPr'
NAME_YQ = 'yQ'
NAME_YD = 'yd'
NAME_YY = 'yy'

HEAD_SIZE = 128


EPS = 1e-06
NEG = -1e30
THETA = 1000000.0


def rms_parts(value_heads_out):
    factor = lax.rsqrt(jnp.mean(value_heads_out * value_heads_out, axis=-1, keepdims=True) + EPS)
    return (value_heads_out * factor, factor)


def norm_back(grad_unit, unit_value, factor):
    return factor * (
        grad_unit - unit_value * jnp.mean(grad_unit * unit_value, axis=-1, keepdims=True)
    )


def rotate(value_heads_out, cos_table, sin_table):
    half_dim = value_heads_out.shape[-1] // 2
    lower_half = value_heads_out[..., :half_dim]
    upper_half = value_heads_out[..., half_dim:]
    return jnp.concatenate(
        [
            lower_half * cos_table - upper_half * sin_table,
            upper_half * cos_table + lower_half * sin_table,
        ],
        axis=-1,
    )


def doc_tables(doc_start):
    row_count = doc_start.shape[0]
    places = jnp.arange(row_count, dtype=jnp.int32)
    begins = lax.cummax(jnp.where(doc_start == 1, places, 0), axis=0)
    offset = (places - begins).astype(jnp.float32)
    frequency = THETA ** (-(jnp.arange(HEAD_SIZE // 2, dtype=jnp.float32) * 2.0 / HEAD_SIZE))
    angles = offset[:, None] * frequency[None, :]
    document_index = jnp.cumsum(doc_start)
    allowed = (document_index[:, None] == document_index[None, :]) & (
        places[:, None] >= places[None, :]
    )
    return (jnp.cos(angles)[:, None, :], jnp.sin(angles)[:, None, :], allowed)


def scores_of(grouped_heads, keys_low, allowed):
    scaled = jnp.einsum(
        NAME_QNGD_KND_NGQK, grouped_heads, keys_low, preferred_element_type=jnp.float32
    ) * HEAD_SIZE ** (-0.5)
    return jnp.where(allowed, scaled, NEG)


def to_owners(fetcher, experts, capacity):
    picked = fetcher(jnp.arange(experts * capacity, dtype=jnp.int32)).reshape(experts, capacity, -1)
    arrived = lax.all_to_all(picked, NAME_EXPERT, split_axis=0, concat_axis=0, tiled=True)
    return arrived


def to_sources(expert_rows, places_sent):
    width = expert_rows.shape[-1]
    returned = lax.all_to_all(expert_rows, NAME_EXPERT, split_axis=0, concat_axis=0, tiled=True)
    return returned.reshape(-1, width)[places_sent].astype(jnp.float32)


def local(
    tokens,
    attn_gain,
    moe_gain,
    query_gain,
    key_gain,
    query_weight,
    key_weight,
    value_matrix,
    output_weight,
    gate_proj,
    up_proj,
    down_proj,
    gate_weights,
    routes,
    doc_start,
    cotangent,
):
    gathered = (
        lax.all_gather(query_weight, NAME_EXPERT, axis=0, tiled=True),
        lax.all_gather(key_weight, NAME_EXPERT, axis=0, tiled=True),
        lax.all_gather(value_matrix, NAME_EXPERT, axis=0, tiled=True),
        lax.all_gather(output_weight, NAME_EXPERT, axis=0, tiled=True),
        lax.all_gather(attn_gain, NAME_EXPERT, axis=0, tiled=True),
        lax.all_gather(moe_gain, NAME_EXPERT, axis=0, tiled=True),
        lax.all_gather(query_gain, NAME_EXPERT, axis=0, tiled=True),
        lax.all_gather(key_gain, NAME_EXPERT, axis=0, tiled=True),
    )
    full_query, full_key, full_value, full_output = (
        gathered[0],
        gathered[1],
        gathered[2],
        gathered[3],
    )
    gain_attn = gathered[4].astype(jnp.float32)
    gain_moe = gathered[5].astype(jnp.float32)
    gain_query = gathered[6].astype(jnp.float32)
    gain_key = gathered[7].astype(jnp.float32)
    cos_table, sin_table, allowed = doc_tables(doc_start)
    tok_rows = tokens.shape[0]
    heads_here = full_query.shape[1] // HEAD_SIZE
    kv_here = full_key.shape[1] // HEAD_SIZE
    query_group_width = heads_here // kv_here
    inputs = tokens.astype(jnp.float32)
    unit_attn, factor_attn = rms_parts(inputs)
    normalized_input = (unit_attn * gain_attn).astype(jnp.bfloat16)
    query_raw = jnp.dot(normalized_input, full_query, preferred_element_type=jnp.float32).reshape(
        tok_rows, heads_here, HEAD_SIZE
    )
    key_unrotated = jnp.dot(normalized_input, full_key, preferred_element_type=jnp.float32).reshape(
        tok_rows, kv_here, HEAD_SIZE
    )
    values_low = (
        jnp.dot(normalized_input, full_value, preferred_element_type=jnp.float32)
        .astype(jnp.bfloat16)
        .reshape(tok_rows, kv_here, HEAD_SIZE)
    )
    query_unit, query_factor = rms_parts(query_raw)
    key_unit, key_factor = rms_parts(key_unrotated)
    queries_low = rotate(query_unit * gain_query, cos_table, sin_table).astype(jnp.bfloat16)
    keys_low = rotate(key_unit * gain_key, cos_table, sin_table).astype(jnp.bfloat16)
    grouped_heads = queries_low.reshape(tok_rows, kv_here, query_group_width, HEAD_SIZE)
    scores = scores_of(grouped_heads, keys_low, allowed)
    row_peak = jnp.max(scores, axis=-1, keepdims=True)
    weights = jnp.exp(scores - row_peak)
    totals = jnp.sum(weights, axis=-1, keepdims=True)
    probs_low = (weights / totals).astype(jnp.bfloat16)
    log_total = row_peak + jnp.log(totals)
    mixed_low = (
        jnp.einsum(NAME_NGQK_KND_QNGD, probs_low, values_low, preferred_element_type=jnp.float32)
        .reshape(tok_rows, heads_here * HEAD_SIZE)
        .astype(jnp.bfloat16)
    )
    attn_part = jnp.einsum(NAME_TH_DH_TD, mixed_low, full_output, preferred_element_type=jnp.float32)
    hidden = inputs + lax.psum(attn_part, NAME_TENSOR)
    unit_moe, factor_moe = rms_parts(hidden)
    normed_moe = (unit_moe * gain_moe).astype(jnp.bfloat16)
    n_devices = lax.axis_size(NAME_EXPERT)
    local_experts = gate_proj.shape[0]
    experts = n_devices * local_experts
    top_count = routes.shape[1]
    assigned = tok_rows * top_count
    capacity = assigned * 5 // (4 * experts)
    chosen = routes.reshape(assigned)
    onehot = (chosen[:, None] == jnp.arange(experts, dtype=jnp.int32)[None, :]).astype(jnp.int32)
    slot_of = jnp.sum((jnp.cumsum(onehot, axis=0) - onehot) * onehot, axis=1)
    places_sent = chosen * capacity + slot_of
    slot_owner = (
        jnp.full((experts * capacity,), assigned, jnp.int32)
        .at[places_sent]
        .set(jnp.arange(assigned, dtype=jnp.int32))
    )
    normed_pad = jnp.concatenate(
        [normed_moe, jnp.zeros((1, normed_moe.shape[1]), jnp.bfloat16)], axis=0
    )

    def fetch_rows(slot_ids):
        return normed_pad[slot_owner[slot_ids] // top_count]

    arrived = to_owners(fetch_rows, experts, capacity).reshape(
        n_devices, local_experts, capacity, -1
    )
    gate_value = jnp.einsum(
        NAME_SLED_LDF_SLEF, arrived, gate_proj, preferred_element_type=jnp.float32
    )
    up_value = jnp.einsum(NAME_SLED_LDF_SLEF, arrived, up_proj, preferred_element_type=jnp.float32)
    hidden_act = (jax.nn.silu(gate_value) * up_value).astype(jnp.bfloat16)
    out_rows = jnp.einsum(
        NAME_SLEF_LFD_SLED, hidden_act, down_proj, preferred_element_type=jnp.float32
    ).astype(jnp.bfloat16)
    per_choice = to_sources(out_rows.reshape(experts, capacity, -1), places_sent).reshape(
        tok_rows, top_count, -1
    )
    moe_part = jnp.sum(gate_weights[:, :, None] * per_choice, axis=1)
    moe_out = lax.psum(moe_part.astype(jnp.bfloat16), NAME_TENSOR).astype(jnp.float32)
    block_out = (hidden + moe_out).astype(jnp.bfloat16)
    upstream = cotangent.astype(jnp.float32)
    gate_part = jnp.sum(per_choice * upstream[:, None, :], axis=-1)
    cot_pad = jnp.concatenate([cotangent, jnp.zeros((1, cotangent.shape[1]), jnp.bfloat16)], axis=0)
    weight_pad = jnp.concatenate(
        [gate_weights.reshape(assigned), jnp.zeros((1,), jnp.float32)], axis=0
    )

    def fetch_grads(slot_ids):
        chosen_slot = slot_owner[slot_ids]
        return (
            weight_pad[chosen_slot][:, None] * cot_pad[chosen_slot // top_count].astype(jnp.float32)
        ).astype(jnp.bfloat16)

    grad_rows = to_owners(fetch_grads, experts, capacity).reshape(
        n_devices, local_experts, capacity, -1
    )
    grad_act = jnp.einsum(
        NAME_SLED_LFD_SLEF, grad_rows, down_proj, preferred_element_type=jnp.float32
    )
    grad_down = jnp.einsum(
        NAME_SLEF_SLED_LFD, hidden_act, grad_rows, preferred_element_type=jnp.float32
    )
    sigmoid_gate = jax.nn.sigmoid(gate_value)
    grad_up_low = (grad_act * gate_value * sigmoid_gate).astype(jnp.bfloat16)
    grad_gate_low = (
        grad_act * up_value * sigmoid_gate * (1.0 + gate_value * (1.0 - sigmoid_gate))
    ).astype(jnp.bfloat16)
    grad_gate_w = jnp.einsum(
        NAME_SLED_SLEF_LDF, arrived, grad_gate_low, preferred_element_type=jnp.float32
    )
    grad_up_w = jnp.einsum(
        NAME_SLED_SLEF_LDF, arrived, grad_up_low, preferred_element_type=jnp.float32
    )
    grad_in = jnp.einsum(
        NAME_SLEF_LDF_SLED, grad_gate_low, gate_proj, preferred_element_type=jnp.float32
    )
    grad_in = (
        grad_in
        + jnp.einsum(NAME_SLEF_LDF_SLED, grad_up_low, up_proj, preferred_element_type=jnp.float32)
    ).astype(jnp.bfloat16)
    grad_choice = to_sources(grad_in.reshape(experts, capacity, -1), places_sent).reshape(
        tok_rows, top_count, -1
    )
    grad_moe_part = jnp.sum(grad_choice, axis=1)
    grad_normed_moe, grad_gates = lax.psum((grad_moe_part, gate_part), NAME_TENSOR)
    grad_moe_gain = jnp.sum(grad_normed_moe * unit_moe, axis=0)
    grad_hidden = upstream + norm_back(grad_normed_moe * gain_moe, unit_moe, factor_moe)
    grad_attn_low = grad_hidden.astype(jnp.bfloat16)
    back_query, back_key, back_value, back_output = (full_query, full_key, full_value, full_output)
    grad_mixed = jnp.einsum(
        NAME_TD_DH_TH, grad_attn_low, back_output, preferred_element_type=jnp.float32
    )
    grad_mixed_low = grad_mixed.astype(jnp.bfloat16).reshape(
        tok_rows, kv_here, query_group_width, HEAD_SIZE
    )
    grad_output_w = jnp.einsum(
        NAME_TD_TH_DH, grad_attn_low, mixed_low, preferred_element_type=jnp.float32
    )
    scores = scores_of(grouped_heads, keys_low, allowed)
    prob_full = jnp.exp(scores - log_total)
    grad_probs = jnp.einsum(
        NAME_QNGD_KND_NGQK, grad_mixed_low, values_low, preferred_element_type=jnp.float32
    )
    grad_values = jnp.einsum(
        NAME_NGQK_QNGD_KND,
        prob_full.astype(jnp.bfloat16),
        grad_mixed_low,
        preferred_element_type=jnp.float32,
    ).astype(jnp.bfloat16)
    row_delta = jnp.sum(prob_full * grad_probs, axis=-1, keepdims=True)
    grad_scores = (prob_full * (grad_probs - row_delta)).astype(jnp.bfloat16)
    score_scale = HEAD_SIZE ** (-0.5)
    grad_queries = (
        jnp.einsum(
            NAME_NGQK_KND_QNGD, grad_scores, keys_low, preferred_element_type=jnp.float32
        ).reshape(tok_rows, heads_here, HEAD_SIZE)
        * score_scale
    )
    grad_keys = (
        jnp.einsum(NAME_NGQK_QNGD_KND, grad_scores, grouped_heads, preferred_element_type=jnp.float32)
        * score_scale
    )
    grad_qhead = rotate(grad_queries, cos_table, -sin_table)
    grad_khead = rotate(grad_keys, cos_table, -sin_table)
    query_gain_part = jnp.sum(grad_qhead * query_unit, axis=(0, 1))
    key_gain_part = jnp.sum(grad_khead * key_unit, axis=(0, 1))
    grad_query_low = (
        norm_back(grad_qhead * gain_query, query_unit, query_factor)
        .astype(jnp.bfloat16)
        .reshape(tok_rows, heads_here * HEAD_SIZE)
    )
    grad_key_low = (
        norm_back(grad_khead * gain_key, key_unit, key_factor)
        .astype(jnp.bfloat16)
        .reshape(tok_rows, kv_here * HEAD_SIZE)
    )
    grad_value_low = grad_values.reshape(tok_rows, kv_here * HEAD_SIZE)
    grad_normed_part = jnp.einsum(
        NAME_TH_DH_TD, grad_query_low, back_query, preferred_element_type=jnp.float32
    )
    grad_normed_part = grad_normed_part + jnp.einsum(
        NAME_TH_DH_TD, grad_key_low, back_key, preferred_element_type=jnp.float32
    )
    grad_normed_part = grad_normed_part + jnp.einsum(
        NAME_TH_DH_TD, grad_value_low, back_value, preferred_element_type=jnp.float32
    )
    grad_query_w = jnp.einsum(
        NAME_TD_TH_DH, normalized_input, grad_query_low, preferred_element_type=jnp.float32
    )
    grad_key_w = jnp.einsum(
        NAME_TD_TH_DH, normalized_input, grad_key_low, preferred_element_type=jnp.float32
    )
    grad_value_w = jnp.einsum(
        NAME_TD_TH_DH, normalized_input, grad_value_low, preferred_element_type=jnp.float32
    )
    grad_normed, query_gain_sum, key_gain_sum = (
        lax.psum(grad_normed_part.astype(jnp.bfloat16), NAME_TENSOR).astype(jnp.float32),
        lax.psum(query_gain_part.astype(jnp.bfloat16), NAME_TENSOR).astype(jnp.float32),
        lax.psum(key_gain_part.astype(jnp.bfloat16), NAME_TENSOR).astype(jnp.float32),
    )
    grad_attn_gain_part = jnp.sum(grad_normed * unit_attn, axis=0)
    grad_tokens = grad_hidden + norm_back(grad_normed * gain_attn, unit_attn, factor_attn)
    shares = (
        lax.psum_scatter(grad_query_w, NAME_EXPERT, scatter_dimension=0, tiled=True),
        lax.psum_scatter(grad_key_w, NAME_EXPERT, scatter_dimension=0, tiled=True),
        lax.psum_scatter(grad_value_w, NAME_EXPERT, scatter_dimension=0, tiled=True),
        lax.psum_scatter(grad_output_w, NAME_EXPERT, scatter_dimension=0, tiled=True),
        lax.psum_scatter(grad_attn_gain_part, NAME_EXPERT, scatter_dimension=0, tiled=True),
        lax.psum_scatter(grad_moe_gain, NAME_EXPERT, scatter_dimension=0, tiled=True),
        lax.psum_scatter(query_gain_sum, NAME_EXPERT, scatter_dimension=0, tiled=True),
        lax.psum_scatter(key_gain_sum, NAME_EXPERT, scatter_dimension=0, tiled=True),
    )
    return (
        block_out,
        grad_tokens,
        shares[0],
        shares[1],
        shares[2],
        shares[3],
        shares[4],
        shares[5],
        shares[6],
        shares[7],
        grad_gate_w,
        grad_up_w,
        grad_down,
        grad_gates,
    )


MESH = pl.DeviceIdType.MESH
ZS, YS, XS = 4, 2, 2

def place():
    e = lax.axis_index(NAME_EXPERT); c = lax.axis_index(NAME_TENSOR)
    return e // 4, (e // 2) % 2, e % 2, c

def ident(z, y, x, c):
    return (z * 4 + y * 2 + x, c)

def greet(share):
    z, y, x, c = place()
    bar = pltpu.get_barrier_semaphore()
    def hello(dev):
        pl.semaphore_signal(bar, inc=1, device_id=dev, device_id_type=MESH)
    hello(ident(z, y, 1 - x, c))
    hello(ident(z, 1 - y, x, c))
    n = 2
    if share:
        hello(ident(z, y, x, 1 - c)); n = 3
    pl.when(z > 0)(lambda: hello(ident(z - 1, y, x, c)))
    pl.when(z < ZS - 1)(lambda: hello(ident(z + 1, y, x, c)))
    pl.semaphore_wait(bar, n + (z > 0).astype(jnp.int32) + (z < ZS - 1).astype(jnp.int32))

def gather_kernel(n, share, *refs):
    ins, outs = refs[:n], refs[n:2 * n]
    stage = refs[2 * n:3 * n]
    ss, rs, ls = refs[3 * n:]
    z, y, x, c = place()
    greet(share)
    rows = [(r.shape[0] // 2 if share else r.shape[0]) for r in ins]
    full = [r.shape[0] for r in ins]
    def start(a, b, part):
        base = (z * 0 + b) * full[a]
        if share:
            base = base + c * rows[a]
        half = rows[a] // 2
        if part == NAME_W:
            return pl.ds(pl.multiple_of(base, 16), rows[a])
        return pl.ds(pl.multiple_of(base + (0 if part == NAME_P else half), 16), half)
    def src_own(a, part):
        half = rows[a] // 2
        base = c * rows[a] if share else 0
        if part == NAME_W:
            return ins[a].at[pl.ds(base, rows[a]), :]
        off = 0 if part == NAME_P else half
        return ins[a].at[pl.ds(base + off, half), :]
    keys = {}
    def num(k):
        return keys.setdefault(k, len(keys))
    def cp(k, a, b, part, dev, own=False):
        i = num(k)
        dst = outs[a].at[start(a, b, part), :]
        src = src_own(a, part) if own else dst
        return pltpu.make_async_remote_copy(src_ref=src, dst_ref=dst, send_sem=ss.at[i, a], recv_sem=rs.at[i, a],
                                            device_id=dev, device_id_type=MESH)
    def each(f):
        for a in range(n):
            f(a)
    xn, yn, zu, zd, sib = ident(z, y, 1 - x, c), ident(z, 1 - y, x, c), ident(z + 1, y, x, c), ident(z - 1, y, x, c), ident(z, y, x, 1 - c)
    def bid(s, yy, xx):
        return s * 4 + yy * 2 + xx
    sends = []
    me = bid(z, y, x)
    locs = []
    def own_in(a):
        return pltpu.make_async_copy(ins[a], stage[a], ls.at[a, 0])
    def own_out(a):
        return pltpu.make_async_copy(stage[a], outs[a].at[pl.ds(pl.multiple_of(me * full[a], 16), full[a]), :], ls.at[a, 1])
    def send(cond, k, b, part, dev, own=False):
        def go():
            each(lambda a: cp(k, a, b, part, dev, own).start())
        if cond is None: go()
        else: pl.when(cond)(go)
        sends.append((cond, k, b, part, dev, own))
    def recv(cond, k, b, part, dev):
        def go():
            each(lambda a: cp(k, a, b, part, dev).wait_recv())
        if cond is None: go()
        else: pl.when(cond)(go)
    send(z < 3, (NAME_U, 0), me, NAME_W, zu, True)
    send(z > 0, (NAME_D, 0), me, NAME_W, zd, True)
    slots = [(0, 0)] + [(d, sg) for d in (1, 2, 3) for sg in (-1, 1)]
    def cond_of(d, sg):
        if d == 0: return None
        return (z - d >= 0) if sg < 0 else (z + d <= 3)
    def A(d, sg):
        s = z + sg * d; cnd = cond_of(d, sg); own = d == 0
        b = bid(s, y, x)
        send(cnd, (NAME_XP, d, sg), b, NAME_P, xn, own)
        send(cnd, (NAME_YQ, d, sg), b, NAME_Q, yn, own)
        send(cnd, (NAME_XQ, d, sg), b, NAME_Q, xn, own)
        send(cnd, (NAME_YP, d, sg), b, NAME_P, yn, own)
        if share and not own:
            send(cnd, (NAME_S0, d, sg), b, NAME_W, sib)
    def B(d, sg):
        s = z + sg * d; cnd = cond_of(d, sg)
        recv(cnd, (NAME_XP, d, sg), bid(s, y, 1 - x), NAME_P, xn)
        send(cnd, (NAME_YPR, d, sg), bid(s, y, 1 - x), NAME_P, yn)
        recv(cnd, (NAME_YQ, d, sg), bid(s, 1 - y, x), NAME_Q, yn)
        send(cnd, (NAME_XQR, d, sg), bid(s, 1 - y, x), NAME_Q, xn)
    def C(d, sg):
        s = z + sg * d; cnd = cond_of(d, sg)
        recv(cnd, (NAME_XQ, d, sg), bid(s, y, 1 - x), NAME_Q, xn)
        if share: send(cnd, (NAME_S1, d, sg), bid(s, y, 1 - x), NAME_W, sib)
        recv(cnd, (NAME_YP, d, sg), bid(s, 1 - y, x), NAME_P, yn)
        if share: send(cnd, (NAME_S2, d, sg), bid(s, 1 - y, x), NAME_W, sib)
        recv(cnd, (NAME_YPR, d, sg), bid(s, 1 - y, 1 - x), NAME_P, yn)
        recv(cnd, (NAME_XQR, d, sg), bid(s, 1 - y, 1 - x), NAME_Q, xn)
        if share: send(cnd, (NAME_S3, d, sg), bid(s, 1 - y, 1 - x), NAME_W, sib)
    A(0, 0)
    each(lambda a: own_in(a).start())
    each(lambda a: own_in(a).wait())
    each(lambda a: own_out(a).start())
    B(0, 0)
    prev = [(0, 0)]
    for d in (1, 2, 3):
        recv(z - d >= 0, (NAME_U, d - 1), bid(z - d, y, x), NAME_W, zd)
        if d < 3:
            send((z - d >= 0) & (z < 3), (NAME_U, d), bid(z - d, y, x), NAME_W, zu)
        A(d, -1)
        recv(z + d <= 3, (NAME_D, d - 1), bid(z + d, y, x), NAME_W, zu)
        if d < 3:
            send((z + d <= 3) & (z > 0), (NAME_D, d), bid(z + d, y, x), NAME_W, zd)
        A(d, 1)
        B(d, -1); B(d, 1)
        for p in prev: C(*p)
        prev = [(d, -1), (d, 1)]
    for p in prev: C(*p)
    each(lambda a: own_out(a).wait())
    if share:
        for d, sg in slots:
            s = z + sg * d; cnd = cond_of(d, sg)
            def sibwait(k, b):
                def go():
                    for a in range(n):
                        i = num(k)
                        r = outs[a].at[pl.ds(pl.multiple_of(b * full[a] + (1 - c) * rows[a], 16), rows[a]), :]
                        pltpu.make_async_remote_copy(src_ref=r, dst_ref=r, send_sem=ss.at[i, a], recv_sem=rs.at[i, a], device_id=sib, device_id_type=MESH).wait_recv()
                if cnd is None: go()
                else: pl.when(cnd)(go)
            if d: sibwait((NAME_S0, d, sg), bid(s, y, x))
            sibwait((NAME_S1, d, sg), bid(s, y, 1 - x))
            sibwait((NAME_S2, d, sg), bid(s, 1 - y, x))
            sibwait((NAME_S3, d, sg), bid(s, 1 - y, 1 - x))
    for cond, k, b, part, dev, own in sends:
        def go():
            each(lambda a: cp(k, a, b, part, dev, own).wait_send())
        if cond is None: go()
        else: pl.when(cond)(go)
    assert len(keys) <= NKEYS, len(keys)

NKEYS = 80
def all_gather_blocks(arrays, cid, share=False):
    n = len(arrays)
    anyspec = pl.BlockSpec(memory_space=pltpu.HBM)
    return pl.pallas_call(
        functools.partial(gather_kernel, n, share),
        out_shape=[jax.ShapeDtypeStruct((16 * a.shape[0], a.shape[1]), a.dtype) for a in arrays],
        in_specs=[anyspec] * n, out_specs=[anyspec] * n,
        scratch_shapes=[pltpu.VMEM(a.shape, a.dtype) for a in arrays] + [
            pltpu.SemaphoreType.DMA((NKEYS, n)), pltpu.SemaphoreType.DMA((NKEYS, n)), pltpu.SemaphoreType.DMA((n, 2))],
        compiler_params=pltpu.CompilerParams(collective_id=cid, has_side_effects=True),
        name=NAME_GATHER_BLOCKS,
    )(*arrays)


SLOTS = [(3, -1), (3, 1), (2, -1), (2, 1), (1, -1), (1, 1), (0, 0)]
CH = 32

def scatter_kernel(part, out, A, SR, RP, RP2, RQ, RQ2, ZU, ZD, ls, ss, rs):
    z, y, x, c = place()
    rows = A.shape[1]; half = rows // 2
    greet(True)
    xn, yn, zu, zd, sib = ident(z, y, 1 - x, c), ident(z, 1 - y, x, c), ident(z + 1, y, x, c), ident(z - 1, y, x, c), ident(z, y, x, 1 - c)
    keys = {}
    def num(k): return keys.setdefault(k, len(keys))
    def cond_of(d, sg):
        if d == 0: return None
        return (z - d >= 0) if sg < 0 else (z + d <= 3)
    def guard(cnd, go):
        if cnd is None: go()
        else: pl.when(cnd)(go)
    sent = []
    def rc(k, src, dst, dev):
        i = num(k)
        return pltpu.make_async_remote_copy(src_ref=src, dst_ref=dst, send_sem=ss.at[i], recv_sem=rs.at[i], device_id=dev, device_id_type=MESH)
    def send(cnd, k, src, dst, dev):
        guard(cnd, lambda: rc(k, src, dst, dev).start())
        sent.append((cnd, k, src, dst, dev))
    def recv(cnd, k, dst, dev):
        guard(cnd, lambda: rc(k, dst, dst, dev).wait_recv())
    def blocks(s):
        b = s * 4
        return b + y * 2 + x, b + y * 2 + 1 - x, b + (1 - y) * 2 + x, b + (1 - y) * 2 + 1 - x
    Ph, Qh = pl.ds(0, half), pl.ds(half, half)
    def part_at(b, cc):
        return part.at[pl.ds(pl.multiple_of(b * 2 * rows + cc * rows, 16), rows), :]
    def load(b):
        return pltpu.make_async_copy(part_at(b, c), A.at[b], ls.at[b])
    for d, sg in SLOTS:
        cnd = cond_of(d, sg); s = z + sg * d
        for q, b in enumerate(blocks(s)):
            guard(cnd, lambda: load(b).start())
            send(cnd, (NAME_SIB, d, sg, q), part_at(b, 1 - c), SR.at[b], sib)
    def sum_into(dst, row0, terms, n=half):
        def step(i, _):
            r = pl.ds(row0 + i * CH, CH)
            acc = dst[r, :].astype(jnp.float32)
            for t, off in terms:
                acc = acc + t[pl.ds(off + i * CH, CH), :].astype(jnp.float32)
            dst[r, :] = acc.astype(dst.dtype)
            return 0
        lax.fori_loop(0, n // CH, step, 0)
    def S1(i):
        d, sg = SLOTS[i]; cnd = cond_of(d, sg); s = z + sg * d
        m, xx, yy, dd = blocks(s)
        def go():
            for q, b in enumerate((m, xx, yy, dd)):
                load(b).wait()
                rc((NAME_SIB, d, sg, q), SR.at[b], SR.at[b], sib).wait_recv()
            sum_into(A.at[dd], 0, [(SR.at[dd], 0)], rows)
        guard(cnd, go)
        send(cnd, (NAME_YD, i), A.at[dd, Ph, :], RP.at[s, 1], yn)
        send(cnd, (NAME_XD, i), A.at[dd, Qh, :], RQ.at[s, 1], xn)
        guard(cnd, lambda: (sum_into(A.at[yy], 0, [(SR.at[yy], 0)]), sum_into(A.at[xx], half, [(SR.at[xx], half)]))and None)
        send(cnd, (NAME_YY, i), A.at[yy, Ph, :], RP.at[s, 0], yn)
        send(cnd, (NAME_XX, i), A.at[xx, Qh, :], RQ.at[s, 0], xn)
    def S2(i):
        d, sg = SLOTS[i]; cnd = cond_of(d, sg); s = z + sg * d
        m, xx, yy, dd = blocks(s)
        recv(cnd, (NAME_YD, i), RP.at[s, 1], yn)
        guard(cnd, lambda: sum_into(A.at[xx], 0, [(SR.at[xx], 0), (RP.at[s, 1], 0)]))
        send(cnd, (NAME_X2, i), A.at[xx, Ph, :], RP2.at[s], xn)
        recv(cnd, (NAME_XD, i), RQ.at[s, 1], xn)
        guard(cnd, lambda: sum_into(A.at[yy], half, [(SR.at[yy], half), (RQ.at[s, 1], 0)]))
        send(cnd, (NAME_Y2, i), A.at[yy, Qh, :], RQ2.at[s], yn)
    def S3(i):
        d, sg = SLOTS[i]; cnd = cond_of(d, sg); s = z + sg * d
        m = blocks(s)[0]
        recv(cnd, (NAME_YY, i), RP.at[s, 0], yn)
        recv(cnd, (NAME_XX, i), RQ.at[s, 0], xn)
        recv(cnd, (NAME_X2, i), RP2.at[s], xn)
        recv(cnd, (NAME_Y2, i), RQ2.at[s], yn)
        base_p = [(SR.at[m], 0), (RP.at[s, 0], 0), (RP2.at[s], 0)]
        base_q = [(SR.at[m], half), (RQ.at[s, 0], 0), (RQ2.at[s], 0)]
        if d:
            back = (z > 0) if sg > 0 else (z < 3)
            Z = ZU if sg > 0 else ZD
            name = NAME_U if sg > 0 else NAME_D
            dn, up = (zd, zu) if sg > 0 else (zu, zd)
            has = d <= 2
            def plain():
                sum_into(A.at[m], 0, base_p); sum_into(A.at[m], half, base_q)
            if has:
                recv(cnd & back, (name, d), Z.at[d], dn)
                pl.when(cnd & back)(lambda: (sum_into(A.at[m], 0, base_p + [(Z.at[d], 0)]), sum_into(A.at[m], half, base_q + [(Z.at[d], half)])) and None)
                pl.when(cnd & jnp.logical_not(back))(plain)
            else:
                pl.when(cnd)(plain)
            send(cnd, (name, d - 1), A.at[m], Z.at[d - 1], up)
        else:
            recv(z > 0, (NAME_U, 0), ZU.at[0], zd)
            recv(z < 3, (NAME_D, 0), ZD.at[0], zu)
            lo = jnp.where(z > 0, 1.0, 0.0); hi = jnp.where(z < 3, 1.0, 0.0)
            def emit(row0, terms, flags):
                def step(i, _):
                    acc = A[m, pl.ds(row0 + i * CH, CH), :].astype(jnp.float32)
                    for t, off in terms:
                        acc = acc + t[pl.ds(off + i * CH, CH), :].astype(jnp.float32)
                    if flags[0]: acc = acc + ZU[0, pl.ds(row0 + i * CH, CH), :].astype(jnp.float32)
                    if flags[1]: acc = acc + ZD[0, pl.ds(row0 + i * CH, CH), :].astype(jnp.float32)
                    out[pl.ds(pl.multiple_of(c * rows + row0 + i * CH, CH), CH), :] = acc
                    return 0
                lax.fori_loop(0, half // CH, step, 0)
            for cc, fl in ((z == 0, (False, True)), (z == 3, (True, False)), ((z > 0) & (z < 3), (True, True))):
                @pl.when(cc)
                def _(fl=fl):
                    emit(0, base_p, fl); emit(half, base_q, fl)
            mine = out.at[pl.ds(pl.multiple_of(c * rows, 16), rows), :]
            other = out.at[pl.ds(pl.multiple_of((1 - c) * rows, 16), rows), :]
            send(None, (NAME_FIN,), mine, mine, sib)
            recv(None, (NAME_FIN,), other, sib)
    n = len(SLOTS)
    for i in range(n + 2):
        if i < n: S1(i)
        if 0 <= i - 1 < n: S2(i - 1)
        if 0 <= i - 2 < n: S3(i - 2)
    for cnd, k, src, dst, dev in sent:
        guard(cnd, lambda: rc(k, src, dst, dev).wait_send())
    assert len(keys) <= NK, len(keys)

NK = 90
def reduce_scatter_rows(part, cid):
    total, width = part.shape
    rows = total // 32
    half = rows // 2
    bf = part.dtype
    return pl.pallas_call(
        scatter_kernel,
        out_shape=jax.ShapeDtypeStruct((2 * rows, width), jnp.float32),
        in_specs=[pl.BlockSpec(memory_space=pltpu.HBM)], out_specs=pl.BlockSpec(memory_space=pltpu.VMEM),
        scratch_shapes=[
            pltpu.VMEM((16, rows, width), bf), pltpu.VMEM((16, rows, width), bf),
            pltpu.VMEM((4, 2, half, width), bf), pltpu.VMEM((4, half, width), bf),
            pltpu.VMEM((4, 2, half, width), bf), pltpu.VMEM((4, half, width), bf),
            pltpu.VMEM((3, rows, width), bf), pltpu.VMEM((3, rows, width), bf),
            pltpu.SemaphoreType.DMA((16,)), pltpu.SemaphoreType.DMA((NK,)), pltpu.SemaphoreType.DMA((NK,))],
        compiler_params=pltpu.CompilerParams(collective_id=cid, has_side_effects=True, vmem_limit_bytes=67043328),
        name=NAME_SCATTER_ROWS,
    )(part)


STEP = 16

def grads_kernel(n, *refs):
    ins, small = refs[:n], refs[n]
    outs, seen = refs[n + 1:2 * n + 1], refs[2 * n + 1]
    A, RP, RP2, RQ, RQ2, ZU, ZD, V, ls, ss, rs, fs, fr = refs[2 * n + 2:]
    z, y, x, c = place()
    rows = A.shape[1]; half = rows // 2
    devices = small.shape[0]
    me = (z * 4 + y * 2 + x) * 2 + c
    widths = [r.shape[1] for r in ins]
    offs = [sum(widths[:a]) for a in range(n)]
    def peer(i):
        p = lax.rem(me + i, devices)
        return p, (p // 2, p % 2)
    bar = pltpu.get_barrier_semaphore()
    def hello(i, _):
        pl.semaphore_signal(bar, inc=1, device_id=peer(i)[1], device_id_type=MESH)
        return 0
    def cond_of(d, sg):
        if d == 0: return None
        return (z - d >= 0) if sg < 0 else (z + d <= 3)
    def guard(cnd, go):
        if cnd is None: go()
        else: pl.when(cnd)(go)
    def blocks(s):
        b = s * 4
        return b + y * 2 + x, b + y * 2 + 1 - x, b + (1 - y) * 2 + x, b + (1 - y) * 2 + 1 - x
    def loads(b):
        return [pltpu.make_async_copy(ins[a].at[pl.ds(pl.multiple_of(b * rows, 16), rows), :],
                                      A.at[b, :, pl.ds(offs[a], widths[a])], ls.at[b, a]) for a in range(n)]
    for d, sg in SLOTS:
        for b in blocks(z + sg * d):
            guard(cond_of(d, sg), lambda: [l.start() for l in loads(b)] and None)
    lax.fori_loop(1, devices, hello, 0)
    pl.semaphore_wait(bar, devices - 1)
    def piece(i, to):
        p, dev = peer(i)
        return pltpu.make_async_remote_copy(src_ref=small.at[p], dst_ref=seen.at[me], send_sem=fs.at[i], recv_sem=fr.at[i],
                                            device_id=dev, device_id_type=MESH)
    def piece_in(i):
        q = lax.rem(me - i + devices, devices)
        return pltpu.make_async_remote_copy(src_ref=small.at[q], dst_ref=seen.at[q], send_sem=fs.at[i], recv_sem=fr.at[i],
                                            device_id=(q // 2, q % 2), device_id_type=MESH)
    def piece_go(i, _):
        piece(i, 0).start(); return 0
    lax.fori_loop(1, devices, piece_go, 0)
    seen[me] = small[me]
    xn, yn, zu, zd = ident(z, y, 1 - x, c), ident(z, 1 - y, x, c), ident(z + 1, y, x, c), ident(z - 1, y, x, c)
    keys = {}
    def num(k): return keys.setdefault(k, len(keys))
    sent = []
    def rc(k, src, dst, dev):
        i = num(k)
        return pltpu.make_async_remote_copy(src_ref=src, dst_ref=dst, send_sem=ss.at[i], recv_sem=rs.at[i], device_id=dev, device_id_type=MESH)
    def send(cnd, k, src, dst, dev):
        guard(cnd, lambda: rc(k, src, dst, dev).start())
        sent.append((cnd, k, src, dst, dev))
    def recv(cnd, k, dst, dev):
        guard(cnd, lambda: rc(k, dst, dst, dev).wait_recv())
    Ph, Qh = pl.ds(0, half), pl.ds(half, half)
    def add_into(store, terms, n_rows=half):
        def step(i, _):
            acc = None
            for t, off in terms:
                v = t[pl.ds(off + i * STEP, STEP), :].astype(jnp.float32)
                acc = v if acc is None else acc + v
            store(i * STEP, acc)
            return 0
        lax.fori_loop(0, n_rows // STEP, step, 0)
    def to(dst, row0):
        def store(r, acc):
            dst[pl.ds(row0 + r, STEP), :] = acc.astype(dst.dtype)
        return store
    def to_outs(row0):
        def store(r, acc):
            for a in range(n):
                outs[a][pl.ds(row0 + r, STEP), :] = acc[:, offs[a]:offs[a] + widths[a]]
        return store
    def S1(i):
        d, sg = SLOTS[i]; cnd = cond_of(d, sg); s = z + sg * d
        m, xx, yy, dd = blocks(s)
        guard(cnd, lambda: [l.wait() for b in (m, xx, yy, dd) for l in loads(b)] and None)
        send(cnd, (NAME_YD, i), A.at[dd, Ph, :], RP.at[s, 1], yn)
        send(cnd, (NAME_XD, i), A.at[dd, Qh, :], RQ.at[s, 1], xn)
        send(cnd, (NAME_YY, i), A.at[yy, Ph, :], RP.at[s, 0], yn)
        send(cnd, (NAME_XX, i), A.at[xx, Qh, :], RQ.at[s, 0], xn)
    def S2(i):
        d, sg = SLOTS[i]; cnd = cond_of(d, sg); s = z + sg * d
        m, xx, yy, dd = blocks(s)
        recv(cnd, (NAME_YD, i), RP.at[s, 1], yn)
        guard(cnd, lambda: add_into(to(A.at[xx], 0), [(A.at[xx], 0), (RP.at[s, 1], 0)]))
        send(cnd, (NAME_X2, i), A.at[xx, Ph, :], RP2.at[s], xn)
        recv(cnd, (NAME_XD, i), RQ.at[s, 1], xn)
        guard(cnd, lambda: add_into(to(A.at[yy], half), [(A.at[yy], half), (RQ.at[s, 1], 0)]))
        send(cnd, (NAME_Y2, i), A.at[yy, Qh, :], RQ2.at[s], yn)
    def S3(i):
        d, sg = SLOTS[i]; cnd = cond_of(d, sg); s = z + sg * d
        m = blocks(s)[0]
        recv(cnd, (NAME_YY, i), RP.at[s, 0], yn)
        recv(cnd, (NAME_XX, i), RQ.at[s, 0], xn)
        recv(cnd, (NAME_X2, i), RP2.at[s], xn)
        recv(cnd, (NAME_Y2, i), RQ2.at[s], yn)
        base_p = [(A.at[m], 0), (RP.at[s, 0], 0), (RP2.at[s], 0)]
        base_q = [(A.at[m], half), (RQ.at[s, 0], 0), (RQ2.at[s], 0)]
        if d:
            slot = s - 1 if sg > 0 else s
            back = (z > 0) if sg > 0 else (z < 3)
            Z, name, dn, up = (ZU, NAME_U, zd, zu) if sg > 0 else (ZD, NAME_D, zu, zd)
            def plain():
                add_into(to(V.at[slot], 0), base_p); add_into(to(V.at[slot], half), base_q)
            if d <= 2:
                recv(cnd & back, (name, d), Z.at[d], dn)
                def carried():
                    add_into(to(V.at[slot], 0), base_p + [(Z.at[d], 0)]); add_into(to(V.at[slot], half), base_q + [(Z.at[d], half)])
                pl.when(cnd & back)(carried)
                pl.when(cnd & jnp.logical_not(back))(plain)
            else:
                pl.when(cnd)(plain)
            send(cnd, (name, d - 1), V.at[slot], Z.at[d - 1], up)
        else:
            recv(z > 0, (NAME_U, 0), ZU.at[0], zd)
            recv(z < 3, (NAME_D, 0), ZD.at[0], zu)
            for cc, zs in ((z == 0, (ZD,)), (z == 3, (ZU,)), ((z > 0) & (z < 3), (ZU, ZD))):
                def emit(zs=zs):
                    add_into(to_outs(0), base_p + [(q.at[0], 0) for q in zs])
                    add_into(to_outs(half), base_q + [(q.at[0], half) for q in zs])
                pl.when(cc)(emit)
    k = len(SLOTS)
    for i in range(k + 2):
        if i < k: S1(i)
        if 0 <= i - 1 < k: S2(i - 1)
        if 0 <= i - 2 < k: S3(i - 2)
    for cnd, key, src, dst, dev in sent:
        guard(cnd, lambda: rc(key, src, dst, dev).wait_send())
    def piece_end(i, _):
        piece(i, 0).wait_send()
        piece_in(i).wait_recv()
        return 0
    lax.fori_loop(1, devices, piece_end, 0)
    assert len(keys) <= NG, len(keys)

NG = 56
def reduce_scatter_grads(parts, small, cid):
    n = len(parts)
    rows = parts[0].shape[0] // (small.shape[0] // 2)
    half = rows // 2
    width = sum(p.shape[1] for p in parts)
    bf, f32 = parts[0].dtype, jnp.float32
    vmem, hbm = pl.BlockSpec(memory_space=pltpu.VMEM), pl.BlockSpec(memory_space=pltpu.HBM)
    res = pl.pallas_call(
        functools.partial(grads_kernel, n),
        out_shape=[jax.ShapeDtypeStruct((rows, p.shape[1]), f32) for p in parts] + [jax.ShapeDtypeStruct(small.shape, f32)],
        in_specs=[hbm] * n + [vmem], out_specs=[vmem] * (n + 1),
        scratch_shapes=[
            pltpu.VMEM((16, rows, width), bf),
            pltpu.VMEM((4, 2, half, width), bf), pltpu.VMEM((4, half, width), bf),
            pltpu.VMEM((4, 2, half, width), bf), pltpu.VMEM((4, half, width), bf),
            pltpu.VMEM((3, rows, width), f32), pltpu.VMEM((3, rows, width), f32), pltpu.VMEM((3, rows, width), f32),
            pltpu.SemaphoreType.DMA((16, n)), pltpu.SemaphoreType.DMA((NG,)), pltpu.SemaphoreType.DMA((NG,)),
            pltpu.SemaphoreType.DMA((small.shape[0],)), pltpu.SemaphoreType.DMA((small.shape[0],))],
        compiler_params=pltpu.CompilerParams(collective_id=cid, has_side_effects=True, vmem_limit_bytes=67043328),
        name=NAME_SCATTER_GRADS,
    )(*parts, small)
    return res[:n], res[n]

def tables(routes_all, weights_all, first, local_experts, capacity):
    n, rows, top = routes_all.shape
    tri = (jnp.arange(rows)[:, None] <= jnp.arange(rows)[None, :]).astype(jnp.bfloat16)
    picks, scale, token_w = [], [], []
    for l in range(local_experts):
        hit = routes_all == (first + l)
        member = jnp.any(hit, axis=-1)
        weight = jnp.sum(jnp.where(hit, weights_all, 0.0), axis=-1)
        rank = jnp.dot(member.astype(jnp.bfloat16), tri, preferred_element_type=jnp.float32).astype(jnp.int32)
        slot = jnp.where(member, rank - 1, -1)
        pick = slot[:, None, :] == jnp.arange(capacity, dtype=jnp.int32)[None, :, None]
        picks.append(pick)
        scale.append(jnp.sum(jnp.where(pick, weight[:, None, :], 0.0), axis=-1, keepdims=True))
    return picks, scale


def local_block(
    tokens, attn_gain, moe_gain, query_gain, key_gain, query_weight, key_weight, value_matrix, output_weight,
    gate_proj, up_proj, down_proj, gate_weights, routes, doc_start, cotangent,
):
    f32, bf16 = jnp.float32, jnp.bfloat16
    tok_rows, width = tokens.shape
    top_count = routes.shape[1]
    n_chips = ZS * YS * XS
    assigned = tok_rows * top_count
    lanes = 128
    list_rows = assigned // lanes
    small = jnp.concatenate(
        [
            attn_gain.astype(f32).reshape(-1, lanes), moe_gain.astype(f32).reshape(-1, lanes),
            jnp.pad(jnp.concatenate([query_gain, key_gain]).astype(f32), (0, lanes - 2 * query_gain.shape[0])).reshape(1, lanes),
            routes.astype(f32).reshape(list_rows, lanes), gate_weights.reshape(list_rows, lanes),
        ], axis=0)
    gain_rows = attn_gain.shape[0] // lanes
    small = jnp.pad(small, ((0, -small.shape[0] % 32), (0, 0)))
    full_query, full_key, full_value, full_output, gathered = all_gather_blocks(
        [query_weight, key_weight, value_matrix, output_weight, small], 1)
    (dy_all,) = all_gather_blocks([cotangent], 2, share=True)
    gathered = gathered.reshape(n_chips, -1, lanes)
    gain_attn = gathered[:, :gain_rows].reshape(-1)
    gain_moe = gathered[:, gain_rows:2 * gain_rows].reshape(-1)
    per = query_gain.shape[0]
    gain_query = gathered[:, 2 * gain_rows, :per].reshape(-1)
    gain_key = gathered[:, 2 * gain_rows, per:2 * per].reshape(-1)
    off = 2 * gain_rows + 1
    routes_all = gathered[:, off:off + list_rows].astype(jnp.int32).reshape(n_chips, tok_rows, top_count)
    weights_all = gathered[:, off + list_rows:off + 2 * list_rows].reshape(n_chips, tok_rows, top_count)

    cos_table, sin_table, allowed = doc_tables(doc_start)
    heads_here = full_query.shape[1] // HEAD_SIZE
    kv_here = full_key.shape[1] // HEAD_SIZE
    query_group_width = heads_here // kv_here
    inputs = tokens.astype(f32)
    unit_attn, factor_attn = rms_parts(inputs)
    normalized_input = (unit_attn * gain_attn).astype(bf16)
    query_raw = jnp.dot(normalized_input, full_query, preferred_element_type=f32).reshape(tok_rows, heads_here, HEAD_SIZE)
    key_unrotated = jnp.dot(normalized_input, full_key, preferred_element_type=f32).reshape(tok_rows, kv_here, HEAD_SIZE)
    values_low = jnp.dot(normalized_input, full_value, preferred_element_type=f32).astype(bf16).reshape(tok_rows, kv_here, HEAD_SIZE)
    query_unit, query_factor = rms_parts(query_raw)
    key_unit, key_factor = rms_parts(key_unrotated)
    queries_low = rotate(query_unit * gain_query, cos_table, sin_table).astype(bf16)
    keys_low = rotate(key_unit * gain_key, cos_table, sin_table).astype(bf16)
    grouped_heads = queries_low.reshape(tok_rows, kv_here, query_group_width, HEAD_SIZE)
    scores = scores_of(grouped_heads, keys_low, allowed)
    row_peak = jnp.max(scores, axis=-1, keepdims=True)
    weights = jnp.exp(scores - row_peak)
    totals = jnp.sum(weights, axis=-1, keepdims=True)
    probs_low = (weights / totals).astype(bf16)
    log_total = row_peak + jnp.log(totals)
    mixed_low = (
        jnp.einsum(NAME_NGQK_KND_QNGD, probs_low, values_low, preferred_element_type=f32)
        .reshape(tok_rows, heads_here * HEAD_SIZE).astype(bf16))
    attn_part = jnp.einsum(NAME_TH_DH_TD, mixed_low, full_output, preferred_element_type=f32)
    hidden = inputs + lax.psum(attn_part, NAME_TENSOR)
    unit_moe, factor_moe = rms_parts(hidden)
    normed_moe = (unit_moe * gain_moe).astype(bf16)

    local_experts = gate_proj.shape[0]
    experts = n_chips * local_experts
    capacity = assigned * 5 // (4 * experts)
    chip = lax.axis_index(NAME_EXPERT)
    picks, scale = tables(routes_all, weights_all, chip * local_experts, local_experts, capacity)
    (x_all,) = all_gather_blocks([normed_moe], 3, share=True)
    x_all = x_all.reshape(n_chips, tok_rows, width)
    dy_all = dy_all.reshape(n_chips, tok_rows, width)
    y_rows, dx_rows, gates_tok, grads = [], [], [], []
    for l in range(local_experts):
        pick = picks[l].astype(bf16)
        def take(source):
            return jnp.einsum(NAME_SJT_STD_SJD, pick, source, preferred_element_type=f32)
        w_slot = scale[l].reshape(-1, 1)
        xs = take(x_all).astype(bf16).reshape(-1, width)
        dys = (scale[l] * take(dy_all)).astype(bf16).reshape(-1, width)
        gate_value = jnp.dot(xs, gate_proj[l], preferred_element_type=f32)
        up_value = jnp.dot(xs, up_proj[l], preferred_element_type=f32)
        sigmoid_gate = jax.nn.sigmoid(gate_value)
        act = (gate_value * sigmoid_gate * up_value).astype(bf16)
        y_rows.append((w_slot * jnp.dot(act, down_proj[l], preferred_element_type=f32)).astype(bf16))
        grad_act = jnp.einsum(NAME_RD_FD_RF, dys, down_proj[l], preferred_element_type=f32)
        gates_slot = jnp.sum(act.astype(f32) * grad_act, axis=-1, keepdims=True) / jnp.where(w_slot > 0, w_slot, 1.0)
        gates_tok.append(jnp.sum(jnp.where(picks[l], gates_slot.reshape(n_chips, capacity, 1), 0.0), axis=1))
        up_low = (grad_act * gate_value * sigmoid_gate).astype(bf16)
        gate_low = (grad_act * up_value * sigmoid_gate * (1.0 + gate_value * (1.0 - sigmoid_gate))).astype(bf16)
        dx = jnp.einsum(NAME_RF_DF_RD, gate_low, gate_proj[l], preferred_element_type=f32)
        dx = dx + jnp.einsum(NAME_RF_DF_RD, up_low, up_proj[l], preferred_element_type=f32)
        dx_rows.append(dx.astype(bf16))
        grads.append((
            jnp.einsum(NAME_RD_RF_DF, xs, gate_low, preferred_element_type=f32),
            jnp.einsum(NAME_RD_RF_DF, xs, up_low, preferred_element_type=f32),
            jnp.einsum(NAME_RF_RD_FD, act, dys, preferred_element_type=f32)))
    pick_both = jnp.concatenate(picks, axis=1).astype(bf16)
    def put(rows):
        both = jnp.concatenate([r.reshape(n_chips, capacity, width) for r in rows], axis=1)
        return jnp.einsum(NAME_SJT_SJD_STD, pick_both, both, preferred_element_type=f32).astype(bf16).reshape(-1, width)
    grad_normed_moe = reduce_scatter_rows(put(dx_rows), 4)
    moe_out = reduce_scatter_rows(put(y_rows), 5)
    grad_gate_w, grad_up_w, grad_down = (jnp.stack([g[i] for g in grads]) for i in range(3))
    block_out = (hidden + moe_out).astype(bf16)
    upstream = cotangent.astype(f32)
    grad_moe_gain = jnp.sum(grad_normed_moe * unit_moe, axis=0)
    grad_hidden = upstream + norm_back(grad_normed_moe * gain_moe, unit_moe, factor_moe)
    grad_attn_low = grad_hidden.astype(bf16)
    grad_mixed = jnp.einsum(NAME_TD_DH_TH, grad_attn_low, full_output, preferred_element_type=f32)
    grad_mixed_low = grad_mixed.astype(bf16).reshape(tok_rows, kv_here, query_group_width, HEAD_SIZE)
    grad_output_w = jnp.einsum(NAME_TD_TH_DH, grad_attn_low, mixed_low, preferred_element_type=f32)
    scores = scores_of(grouped_heads, keys_low, allowed)
    prob_full = jnp.exp(scores - log_total)
    grad_probs = jnp.einsum(NAME_QNGD_KND_NGQK, grad_mixed_low, values_low, preferred_element_type=f32)
    grad_values = jnp.einsum(
        NAME_NGQK_QNGD_KND, prob_full.astype(bf16), grad_mixed_low, preferred_element_type=f32).astype(bf16)
    row_delta = jnp.sum(prob_full * grad_probs, axis=-1, keepdims=True)
    grad_scores = (prob_full * (grad_probs - row_delta)).astype(bf16)
    score_scale = HEAD_SIZE ** (-0.5)
    grad_queries = (
        jnp.einsum(NAME_NGQK_KND_QNGD, grad_scores, keys_low, preferred_element_type=f32)
        .reshape(tok_rows, heads_here, HEAD_SIZE) * score_scale)
    grad_keys = jnp.einsum(NAME_NGQK_QNGD_KND, grad_scores, grouped_heads, preferred_element_type=f32) * score_scale
    grad_qhead = rotate(grad_queries, cos_table, -sin_table)
    grad_khead = rotate(grad_keys, cos_table, -sin_table)
    query_gain_part = jnp.sum(grad_qhead * query_unit, axis=(0, 1))
    key_gain_part = jnp.sum(grad_khead * key_unit, axis=(0, 1))
    grad_query_low = norm_back(grad_qhead * gain_query, query_unit, query_factor).astype(bf16).reshape(tok_rows, -1)
    grad_key_low = norm_back(grad_khead * gain_key, key_unit, key_factor).astype(bf16).reshape(tok_rows, -1)
    grad_value_low = grad_values.reshape(tok_rows, -1)
    grad_normed_part = jnp.einsum(NAME_TH_DH_TD, grad_query_low, full_query, preferred_element_type=f32)
    grad_normed_part = grad_normed_part + jnp.einsum(NAME_TH_DH_TD, grad_key_low, full_key, preferred_element_type=f32)
    grad_normed_part = grad_normed_part + jnp.einsum(NAME_TH_DH_TD, grad_value_low, full_value, preferred_element_type=f32)
    grad_normed = lax.psum(grad_normed_part.astype(bf16), NAME_TENSOR).astype(f32)
    grad_attn_gain_part = jnp.sum(grad_normed * unit_attn, axis=0)
    grad_tokens = grad_hidden + norm_back(grad_normed * gain_attn, unit_attn, factor_attn)

    def weight_grad(left, right):
        return jnp.dot(left.T, right, preferred_element_type=f32).astype(bf16)
    gates_rows = local_experts * tok_rows // lanes
    head_row = jnp.concatenate([query_gain_part.reshape(n_chips, per), key_gain_part.reshape(n_chips, per)], axis=1)
    pieces = jnp.concatenate(
        [
            jnp.stack(gates_tok, axis=1).reshape(n_chips, gates_rows, lanes),
            grad_attn_gain_part.reshape(n_chips, gain_rows, lanes), grad_moe_gain.reshape(n_chips, gain_rows, lanes),
            jnp.pad(head_row, ((0, 0), (0, lanes - 2 * per)))[:, None, :],
        ], axis=1)
    pieces = jnp.repeat(jnp.pad(pieces, ((0, 0), (0, -pieces.shape[1] % 8), (0, 0))), 2, axis=0)
    shares, seen = reduce_scatter_grads(
        [weight_grad(normalized_input, grad_query_low), weight_grad(normalized_input, grad_key_low),
         weight_grad(normalized_input, grad_value_low), weight_grad(grad_attn_low, mixed_low)], pieces, 6)
    gates_back = jnp.sum(seen[:, :gates_rows].reshape(n_chips, 2, local_experts, tok_rows), axis=1).reshape(experts, tok_rows)
    grad_gates = jnp.sum(
        jnp.where(routes[:, :, None] == jnp.arange(experts, dtype=jnp.int32), gates_back.T[:, None, :], 0.0), axis=-1)
    gains = jnp.sum(seen[:, gates_rows:], axis=0)
    own_attn = 0.5 * gains[:gain_rows].reshape(-1)
    own_moe = 0.5 * gains[gain_rows:2 * gain_rows].reshape(-1)
    head_gains = gains[2 * gain_rows]
    return (
        block_out, grad_tokens, *shares,
        own_attn, own_moe, head_gains[:per], head_gains[per:2 * per],
        grad_gate_w, grad_up_w, grad_down, grad_gates,
    )


def solution(mesh):
    wide = mesh.shape[NAME_EXPERT] == ZS * YS * XS and mesh.shape[NAME_TENSOR] == 2
    return jax.shard_map(
        local_block if wide else local,
        mesh=mesh,
        in_specs=(
            P(NAME_EXPERT, None),
            P(NAME_EXPERT),
            P(NAME_EXPERT),
            P(NAME_EXPERT),
            P(NAME_EXPERT),
            P(NAME_EXPERT, NAME_TENSOR),
            P(NAME_EXPERT, NAME_TENSOR),
            P(NAME_EXPERT, NAME_TENSOR),
            P(NAME_EXPERT, NAME_TENSOR),
            P(NAME_EXPERT, None, NAME_TENSOR),
            P(NAME_EXPERT, None, NAME_TENSOR),
            P(NAME_EXPERT, NAME_TENSOR, None),
            P(NAME_EXPERT, None),
            P(NAME_EXPERT, None),
            P(NAME_EXPERT),
            P(NAME_EXPERT, None),
        ),
        out_specs=(
            P(NAME_EXPERT, None),
            P(NAME_EXPERT, None),
            P(NAME_EXPERT, NAME_TENSOR),
            P(NAME_EXPERT, NAME_TENSOR),
            P(NAME_EXPERT, NAME_TENSOR),
            P(NAME_EXPERT, NAME_TENSOR),
            P(NAME_EXPERT),
            P(NAME_EXPERT),
            P(NAME_EXPERT),
            P(NAME_EXPERT),
            P(NAME_EXPERT, None, NAME_TENSOR),
            P(NAME_EXPERT, None, NAME_TENSOR),
            P(NAME_EXPERT, NAME_TENSOR, None),
            P(NAME_EXPERT, None),
        ),
        check_vma=False,
    )
```
